512 devices in a mesh: lat: 64 (over y, z), ma: 8 (over x, core).
Axes of the slice: x: 4, y: 8, z: 8, core: 2. Of those that a mesh axis runs over, the one named last changes fastest.
Arguments:
- pair_wave: int32 [360], replicated, may hold values from 0 to 359, each once
- legendre: bfloat16 [360, 640, 768], P('ma', 'lat'), may hold values from -0.0078125 to 0.0078125
- coefs: bfloat16 [360, 768, 168], P('ma', 'lat'), may hold values from -6 to 6
Outputs:
- noise: float32 [53760, 1440], P(('lat', 'ma'))
The draws below stay inside these ranges and needn't reach their ends.
Inputs may be any that keep to these rules, and one draw needn't show every extreme that they name: Slot q holds wavenumbers pair_wave[q] and 719 - pair_wave[q]; every value appears once.
All inputs are finite; a program needn't handle non-finite values.
Results may differ from the reference program's by a relative error of at most 0.0003.
Values may be sent and summed in bfloat16 or wider, within the bound.
A program may use at most 64 MiB of HBM per device.

```python
import math
import jax
import jax.numpy as jnp
from jax import lax

DEG = 720
LON = 1440
CH = 84
LAT_DEV = 10
PAIRS = 360
RROWS = 768
COLS = 168
LATS = 640
N_LAT = 64
N_MA = 8


def level_of(key, dims, split, smallest, high):
    factor_of = 1.0
    for axis_at, shards_of in split:
        draws = jax.random.uniform(jax.random.fold_in(jax.random.fold_in(key, 6), axis_at), (shards_of,), jnp.float32, smallest / len(split), high / len(split))
        factor_of = factor_of * jnp.repeat(jnp.exp(draws), dims[axis_at] // shards_of).reshape((-1,) + (1,) * (len(dims) - 1 - axis_at))
    return factor_of


def noise(stream_key, extent, deviation, most, shards=(), kind=jnp.bfloat16):
    values = jax.random.normal(stream_key, extent, jnp.float32) * deviation
    if len(shards) > 0:
        values = level_of(stream_key, extent, shards, -0.22, 0.18) * values
    return jnp.clip(values, min=-most, max=most).astype(kind)


def setup_inputs(seed: int = 0) -> dict:
    key_list = jax.random.split(jax.random.key(seed), 4)
    pair_wave = jax.random.permutation(key_list[0], PAIRS).astype(jnp.int32)
    legendre = noise(key_list[1], (PAIRS, LATS, RROWS), (RROWS * DEG) ** -0.5, 0.0078125, ((0, 8), (1, 64)))
    coefs = noise(key_list[2], (PAIRS, RROWS, COLS), 1.0, 6.0, ((0, 8), (1, 64)))
    return dict(pair_wave=pair_wave, legendre=legendre, coefs=coefs)


def chain_table(table, wave_ids, degree_top):
    row_count = table.shape[2]
    row_ids = jnp.arange(row_count, dtype=jnp.int32)[None, :]
    split_row = (degree_top - wave_ids).astype(jnp.int32)[:, None]
    inside = row_ids < split_row
    outside = (row_ids >= split_row) & (row_ids <= degree_top)
    masks = jnp.stack([inside, outside], axis=1)
    return jnp.where(masks[:, :, None, :], table[:, None, :, :], jnp.zeros((), table.dtype))


def fourier_basis(pair_wave, degree_top, lon_count):
    orders = jnp.stack([pair_wave, degree_top - 1 - pair_wave], axis=1).astype(jnp.int32)
    positions = jnp.arange(lon_count, dtype=jnp.int32)
    phase_int = (orders[:, :, None] * positions[None, None, :]) % lon_count
    radians = (2.0 * math.pi / lon_count) * phase_int.astype(jnp.float32)
    weight = jnp.where(orders == 0, 1.0, 2.0).astype(jnp.float32)[:, :, None]
    real_row = weight * jnp.cos(radians)
    imag_row = -weight * jnp.sin(radians)
    return jnp.stack([real_row, imag_row], axis=2).reshape(-1, lon_count)


def reference(pair_wave, legendre, coefs):
    pair_count = pair_wave.shape[0]
    row_count = coefs.shape[1]
    lat_total = LAT_DEV * N_LAT
    slot_count = pair_count // N_MA

    def group_spectra(packed):
        wave_ids, group_table, group_coefs = packed
        masked = chain_table(group_table, wave_ids, DEG)
        return jnp.einsum('qeir,qrc->qeic', masked.astype(jnp.float32), group_coefs.astype(jnp.float32), precision=lax.Precision.HIGHEST)

    spectra = lax.map(group_spectra, (pair_wave.reshape(N_MA, slot_count), legendre.reshape(N_MA, slot_count, lat_total, row_count), coefs.reshape(N_MA, slot_count, row_count, coefs.shape[2])))
    spectra = spectra.reshape(pair_count, 2, lat_total, 2, CH)
    fourier_rows = jnp.transpose(spectra, (0, 1, 3, 2, 4)).reshape(4 * pair_count, lat_total * CH)
    synth_basis = fourier_basis(pair_wave, DEG, LON)
    return lax.dot_general(fourier_rows, synth_basis, (((0,), (0,)), ((), ())), precision=lax.Precision.HIGHEST)
```

```python
import math

import jax
import jax.numpy as jnp
import numpy as np
from jax import lax
from jax.experimental import pallas as pl
from jax.experimental.pallas import tpu as pltpu
from jax.sharding import Mesh
from jax.sharding import PartitionSpec as P

DEG = 720
LON = 1440
HALF = LON // 2
CH = 84
LAT = 10
SLOTS = 45
PER = 6
N = 8
ROWS = 105
RR = 768
F32 = jnp.float32
BF = jnp.bfloat16
MESH_ID = pl.DeviceIdType.MESH
FAR_FIRST = (4, 3, 5, 2, 6, 1, 7)
STRIDE = 88


def half_angle_fit():
    t = np.cos(np.linspace(0, np.pi, 4001)) * (np.pi / 2)
    sin_c = np.linalg.lstsq(np.stack([t ** (2 * i + 1) for i in range(5)], 1), np.sin(t), rcond=None)[0]
    cos_c = np.linalg.lstsq(np.stack([t ** (2 * i) for i in range(6)], 1), np.cos(t), rcond=None)[0]
    return [float(v) for v in sin_c], [float(v) for v in cos_c]


SIN_C, COS_C = half_angle_fit()


def horner(coefs, square):
    total = jnp.full_like(square, coefs[-1])
    for value in coefs[-2::-1]:
        total = total * square + value
    return total


def wave_rows(waves, weight, lon_at):
    product = waves * lon_at
    turns = jnp.round(product * (1.0 / LON))
    half = (product - turns * float(LON)) * (math.pi / LON)
    square = half * half
    sine = half * horner(SIN_C, square)
    cosine = horner(COS_C, square)
    twice = (2.0 * weight) * sine
    return weight - twice * sine, -twice * cosine


def split_bf16(x):
    high = x.astype(BF)
    return high, (x - high.astype(F32)).astype(BF)


def kernel(
    pw, leg_hbm, cf_hbm, out,
    leg, cf, cbuf, csend, crecv, gat, lbuf, lsend, lrecv, ltail, fbuf, fsend, frecv, fdec, ucol, bas,
    in_sem, own_sem, csem, lsem, fsem, ring_s, ring_r,
):
    y, z = lax.axis_index("y"), lax.axis_index("z")
    m = 2 * lax.axis_index("x") + lax.axis_index("c")

    def device(y_at, z_at, m_at):
        return (y_at, z_at, m_at // 2, m_at % 2)

    barrier = pltpu.get_barrier_semaphore()
    peers = [device((y + 1) % N, z, m), device((y + N - 1) % N, z, m)]
    peers += [device(y, (z + t) % N, m) for t in FAR_FIRST]
    peers += [device(y, z, (m + t) % N) for t in FAR_FIRST]
    for peer in peers:
        pl.semaphore_signal(barrier, inc=1, device_id=peer, device_id_type=MESH_ID)
    cf_in = pltpu.make_async_copy(cf_hbm, cf, in_sem.at[0])
    leg_in = pltpu.make_async_copy(leg_hbm, leg, in_sem.at[1])
    cf_in.start()
    leg_in.start()

    def slot_tile(ref, row, j):
        count = min(8, SLOTS - 8 * j)
        tile = ref[row, 8 * j : 8 * j + count, :].astype(F32)
        if count < 8:
            tile = jnp.concatenate([tile, jnp.zeros((8 - count, tile.shape[1]), F32)], 0)
        return tile

    cf_in.wait()
    for r in range(12):
        for g in range(2):
            tiles = [slot_tile(cf, r, 3 * g + k) for k in range(3)]
            at = 8 * (8 * r + 4 * g)
            for k in range(3):
                cbuf[at + 8 * k : at + 8 * k + 8, :] = tiles[k][:, :128]
            rest = [t[:, 128:] for t in tiles] + [jnp.zeros((8, 8), F32)]
            cbuf[at + 24 : at + 32, :] = jnp.concatenate(rest, 1)
    for d in range(N):
        csend[d] = cbuf[pl.ds(d, 96, stride=8), :].astype(BF)
    leg_in.wait()
    for i in range(LAT):
        for j in range(PER):
            at = 8 * (8 * j + i if i < 8 else 48 + 2 * j + i - 8)
            tile = slot_tile(leg, i, j)
            for l in range(6):
                lbuf[l, at : at + 8, :] = tile[:, 128 * l : 128 * l + 128]

    pl.semaphore_wait(barrier, len(peers))

    own_c = pltpu.make_async_copy(csend.at[z], crecv.at[z], own_sem.at[0])
    own_c.start()
    for t in FAR_FIRST:
        to = (z + t) % N
        pltpu.make_async_remote_copy(
            csend.at[to], crecv.at[z], csem.at[0], csem.at[1], device_id=device(y, to, m), device_id_type=MESH_ID
        ).start()

    def send_leg(to):
        pltpu.make_async_remote_copy(
            lsend.at[to], lrecv.at[z], lsem.at[0], lsem.at[1], device_id=device(y, to, m), device_id_type=MESH_ID
        ).start()

    for n, t in enumerate(FAR_FIRST + (0,)):
        to = (z + t) % N
        for l in range(6):
            lsend[to, :, 128 * l : 128 * l + 128] = lbuf[l, pl.ds(to, 60, stride=8), :].astype(BF)
        if n >= 1:
            send_leg((z + FAR_FIRST[n - 1]) % N)
    own_l = pltpu.make_async_copy(lsend.at[z], lrecv.at[z], own_sem.at[1])

    @pl.loop(0, PER * N)
    def _(tile):
        first = SLOTS * (tile % N) + 8 * (tile // N)
        rows = [jnp.full((1, 128), pw[jnp.minimum(first + d, 359)].astype(F32)) for d in range(8)]
        ucol[pl.ds(pl.multiple_of(tile * 8, 8), 8), :] = jnp.concatenate(rows, 0)

    own_l.start()
    lane = lax.broadcasted_iota(jnp.int32, (16, 128), 1).astype(F32)

    def make_basis(first, last):
        @pl.loop(first, last)
        def _(block):
            at = pl.multiple_of(block * 16, 16)
            u = ucol[pl.ds(at, 16), :]
            odd = u - 2.0 * jnp.floor(u * 0.5) > 0.5
            even_wave = jnp.where(odd, float(DEG - 1) - u, u)
            weight = jnp.where(even_wave == 0.0, 1.0, 2.0)
            for h, (wave, wt) in enumerate(((even_wave, weight), (float(DEG - 1) - even_wave, 2.0))):
                for l in range(6):
                    pair = wave_rows(wave, wt, lane + 128.0 * l)
                    for e in range(2):
                        high, low = split_bf16(pair[e])
                        to = pl.multiple_of(384 * e + at, 16)
                        bas[h, 0, pl.ds(to, 16), 128 * l : 128 * l + 128] = high
                        bas[h, 1, pl.ds(to, 16), 128 * l : 128 * l + 128] = low

    make_basis(0, 8)

    def wait_bytes(ref, sem):
        pltpu.make_async_copy(ref, ref, sem).wait()

    own_c.wait()
    wait_bytes(crecv.at[pl.ds(0, 7)], csem.at[1])
    for s in range(N):
        cbuf[96 * s : 96 * s + 96, :] = crecv[s].astype(F32)
    for blk in range(8):
        gat[y, blk] = cbuf[pl.ds(blk, 96, stride=8), :].astype(BF)

    def ring(way, step, half):
        origin = (y - step + N) % N if way == 0 else (y + step) % N
        part = gat.at[origin, pl.ds(4 * half, 4)]
        to = (y + 1) % N if way == 0 else (y + N - 1) % N
        return pltpu.make_async_remote_copy(
            part, part, ring_s.at[way, step, half], ring_r.at[way, step, half],
            device_id=device(to, z, m), device_id_type=MESH_ID,
        )

    for half in range(2):
        for way in range(2):
            ring(way, 0, half).start()
    done = 8
    for step in range(1, 4):
        for half in range(2):
            if done < 24:
                make_basis(done, min(done + 3, 24))
                done = min(done + 3, 24)
            for way in range(2):
                if step < 3 or way == half:
                    ring(way, step - 1, half).wait_recv()
                    ring(way, step, half).start()
    if done < 24:
        make_basis(done, 24)
    own_l.wait()
    wait_bytes(lrecv.at[pl.ds(0, 7)], lsem.at[1])
    for s in range(N):
        for l in range(6):
            ltail[l, 16 * s : 16 * s + 12, :] = lrecv[s, 48:60, 128 * l : 128 * l + 128].astype(F32)
    ring(0, 2, 1).wait_recv()
    ring(1, 2, 0).wait_recv()
    ring(0, 3, 0).wait_recv()
    ring(1, 3, 1).wait_recv()

    row_at = lax.broadcasted_iota(jnp.int32, (1, RR), 1)
    lane80 = lax.broadcasted_iota(jnp.int32, (80, 128), 1)
    for j in range(PER):
        u = pw[SLOTS * m + jnp.minimum(8 * j + z, SLOTS - 1)]
        cut = DEG - u
        odd = lax.rem(u, 2)
        low = (row_at < cut).astype(F32)
        high = (row_at <= DEG).astype(F32) - low
        swap = odd.astype(F32)
        masks = [(low + swap * (high - low)).astype(BF), (high + swap * (low - high)).astype(BF)]
        main = lrecv[:, 8 * j : 8 * j + 8, :].reshape(64, RR)
        tail = [[ltail[l, pl.ds(2 * j + k, 8, stride=16), :] for l in range(6)] for k in range(2)]
        tail = jnp.concatenate([jnp.concatenate(t, 1) for t in tail], 0)
        table = jnp.concatenate([main, tail.astype(BF)], 0)
        lhs = jnp.concatenate([table * masks[0], table * masks[1]], 0)
        g, k = divmod(j, 3)
        rhs = jnp.concatenate([gat[:, 4 * g + k].reshape(RR, 128), gat[:, 4 * g + 3].reshape(RR, 128)], 1)
        sums = jnp.dot(lhs, rhs, preferred_element_type=F32)
        for h in range(2):
            first = sums[80 * h : 80 * h + 80, :128]
            second = sums[80 * h : 80 * h + 80, 128:]
            imag = jnp.where(
                lane80 < 44, pltpu.roll(first, 44, axis=1), pltpu.roll(second, (44 - 40 * k) % 128, axis=1)
            )
            for e, value in enumerate((first, imag)):
                at = (12 * h + 6 * e + j) * STRIDE
                fbuf[at : at + 80, :] = value

    lane24 = lax.broadcasted_iota(jnp.int32, (24, 128), 1)

    def pack(to):
        lats = []
        for i in range(LAT):
            at = 8 * to + i if i < 8 else 64 + 8 * (i - 8) + to
            lats.append(fbuf[pl.ds(at, 24, stride=STRIDE), :])
        for k in range(N):
            i, skip = k + k // 4, 21 * (k % 4)
            keep = CH - skip
            first = pltpu.roll(lats[i], 128 - skip, axis=1) if skip else lats[i]
            window = jnp.where(lane24 < keep, first, pltpu.roll(lats[i + 1], keep, axis=1))
            window = jnp.where(lane24 < ROWS, window, 0.0)
            most = jnp.max(jnp.abs(window), axis=1, keepdims=True)
            level = jnp.ceil(jnp.log2(jnp.maximum(most, 1e-30)))
            scaled = jnp.clip(jnp.round(window * jnp.exp2(15.0 - level)), -32767.0, 32767.0)
            coded = jnp.where(lane24 < ROWS, scaled, jnp.broadcast_to(level, (24, 128)))
            fsend[to, k] = coded.astype(jnp.int32).astype(jnp.int16)

    def send_f(to):
        for t in range(N):
            m_to = (m + t) % N
            pltpu.make_async_remote_copy(
                fsend.at[to, m_to], frecv.at[m * N + z], fsem.at[0], fsem.at[1],
                device_id=device(y, to, m_to), device_id_type=MESH_ID,
            ).start()

    for n, t in enumerate(FAR_FIRST + (0,)):
        pack((z + t) % N)
        if n >= 1:
            send_f((z + FAR_FIRST[n - 1]) % N)
    for t in range(1, N):
        m_to = (m + t) % N
        pltpu.make_async_remote_copy(
            fsend.at[z, m_to], frecv.at[m * N + z], fsem.at[0], fsem.at[1],
            device_id=device(y, z, m_to), device_id_type=MESH_ID,
        ).start()
    own_f = pltpu.make_async_copy(fsend.at[z, m], frecv.at[m * N + z], own_sem.at[2])
    own_f.start()

    wait_bytes(csend.at[pl.ds(0, 7)], csem.at[0])
    wait_bytes(lsend.at[pl.ds(0, 7)], lsem.at[0])
    for way in range(2):
        for step in range(4):
            for half in range(2):
                if step < 3 or way == half:
                    ring(way, step, half).wait_send()
    own_f.wait()
    wait_bytes(frecv.at[pl.ds(0, 63)], fsem.at[1])

    lane192 = lax.broadcasted_iota(jnp.int32, (192, 128), 1)

    @pl.loop(0, 8)
    def _(part):
        coded = frecv[pl.ds(part * 8, 8)].astype(jnp.int32).astype(F32).reshape(192, 128)
        scale = jnp.exp2(coded[:, 127:128] - 15.0)
        fdec[pl.ds(pl.multiple_of(part * 192, 8), 192), :] = jnp.where(lane192 < ROWS, coded * scale, 0.0)

    lhs = []
    for h in range(2):
        rows = jnp.concatenate([fdec[pl.ds(12 * h + t, 64, stride=24), :] for t in range(12)], 0)
        high, low = split_bf16(jnp.transpose(rows))
        lhs.append((high, jnp.concatenate([high, low], 0)))
    for l in range(3):
        at = slice(256 * l, 256 * l + 256)
        part = []
        for h in range(2):
            high, both = lhs[h]
            wide = jnp.dot(both, bas[h, 0, :, at], preferred_element_type=F32)
            part.append(
                wide[:128] + wide[128:] + jnp.dot(high, bas[h, 1, :, at], preferred_element_type=F32)
            )
        count = min(256, HALF - 256 * l)
        out[:, 256 * l : 256 * l + count] = (part[0] + part[1])[:ROWS, :count]
        out[:, HALF + 256 * l : HALF + 256 * l + count] = (part[0] - part[1])[:ROWS, :count]
    wait_bytes(frecv.at[pl.ds(0, 63)], fsem.at[0])


def body(pair_wave, legendre, coefs):
    i16 = jnp.int16
    return pl.pallas_call(
        kernel,
        out_shape=jax.ShapeDtypeStruct((ROWS, LON), F32),
        in_specs=[
            pl.BlockSpec(memory_space=pltpu.SMEM),
            pl.BlockSpec(memory_space=pl.ANY),
            pl.BlockSpec(memory_space=pl.ANY),
        ],
        out_specs=pl.BlockSpec(memory_space=pltpu.VMEM),
        scratch_shapes=[
            pltpu.VMEM((LAT, SLOTS, RR), BF),
            pltpu.VMEM((12, SLOTS, 2 * CH), BF),
            pltpu.VMEM((768, 128), F32),
            pltpu.VMEM((N, 96, 128), BF),
            pltpu.VMEM((N, 96, 128), BF),
            pltpu.VMEM((N, 8, 96, 128), BF),
            pltpu.VMEM((6, 480, 128), F32),
            pltpu.VMEM((N, 60, RR), BF),
            pltpu.VMEM((N, 60, RR), BF),
            pltpu.VMEM((6, 128, 128), F32),
            pltpu.VMEM((24 * STRIDE, 128), F32),
            pltpu.VMEM((N, N, 24, 128), i16),
            pltpu.VMEM((N * N, 24, 128), i16),
            pltpu.VMEM((N * N * 24, 128), F32),
            pltpu.VMEM((384, 128), F32),
            pltpu.VMEM((2, 2, RR, RR), BF),
            pltpu.SemaphoreType.DMA((2,)),
            pltpu.SemaphoreType.DMA((3,)),
            pltpu.SemaphoreType.DMA((2,)),
            pltpu.SemaphoreType.DMA((2,)),
            pltpu.SemaphoreType.DMA((2,)),
            pltpu.SemaphoreType.DMA((2, 4, 2)),
            pltpu.SemaphoreType.DMA((2, 4, 2)),
        ],
        compiler_params=pltpu.CompilerParams(collective_id=0, has_side_effects=True, vmem_limit_bytes=40 << 20),
    )(pair_wave, jnp.transpose(legendre, (1, 0, 2)), jnp.transpose(coefs, (1, 0, 2)))


def solution(mesh):
    split = Mesh(mesh.devices.reshape(N, N, 4, 2), ("y", "z", "x", "c"))
    placed = (P(), P(("x", "c"), ("y", "z"), None), P(("x", "c"), ("y", "z"), None))
    return jax.shard_map(
        body, mesh=split, in_specs=placed, out_specs=P(("y", "z", "x", "c"), None), check_vma=False
    )
```

```python
import math

import jax
import jax.numpy as jnp
import numpy as np
from jax import lax
from jax.experimental import pallas as pl
from jax.experimental.pallas import tpu as pltpu
from jax.sharding import Mesh
from jax.sharding import PartitionSpec as P

DEG = 720
LON = 1440
HALF = LON // 2
CH = 84
LAT = 10
SLOTS = 45
PER = 6
N = 8
ROWS = 105
RR = 768
F32 = jnp.float32
BF = jnp.bfloat16
MESH_ID = pl.DeviceIdType.MESH
FAR_FIRST = (4, 3, 5, 2, 6, 1, 7)
STRIDE = 88
EARLY = 8
SHRINK = 0.9999


def half_angle_fit():
    t = np.cos(np.linspace(0, np.pi, 4001)) * (np.pi / 2)
    sin_c = np.linalg.lstsq(np.stack([t ** (2 * i + 1) for i in range(5)], 1), np.sin(t), rcond=None)[0]
    cos_c = np.linalg.lstsq(np.stack([t ** (2 * i) for i in range(6)], 1), np.cos(t), rcond=None)[0]
    return [float(v) for v in sin_c], [float(v) for v in cos_c]


SIN_C, COS_C = half_angle_fit()


def horner(coefs, square):
    total = jnp.full_like(square, coefs[-1])
    for value in coefs[-2::-1]:
        total = total * square + value
    return total


def wave_rows(waves, weight, lon_at):
    product = waves * lon_at
    turns = jnp.round(product * (1.0 / LON))
    half = (product - turns * float(LON)) * (math.pi / LON)
    square = half * half
    sine = half * horner(SIN_C, square)
    cosine = horner(COS_C, square)
    twice = (2.0 * weight) * sine
    return weight - twice * sine, -twice * cosine


def split_bf16(x):
    high = x.astype(BF)
    return high, (x - high.astype(F32)).astype(BF)


def kernel(
    pw_hbm, leg_hbm, cf_hbm, out,
    pw, leg, cf, cbuf, csend, crecv, gat, lbuf, lsend, lrecv, ltail, fbuf, fsend, frecv, fdec, ucol, bas,
    in_sem, own_sem, csem, lsem, fsem, ring_s, ring_r,
):
    y, z = lax.axis_index("y"), lax.axis_index("z")
    m = 2 * lax.axis_index("x") + lax.axis_index("c")

    def device(y_at, z_at, m_at):
        return (y_at, z_at, m_at // 2, m_at % 2)

    barrier = pltpu.get_barrier_semaphore()
    peers = [device((y + 1) % N, z, m), device((y + N - 1) % N, z, m)]
    peers += [device(y, (z + t) % N, m) for t in FAR_FIRST]
    peers += [device(y, z, (m + t) % N) for t in FAR_FIRST]
    for peer in peers:
        pl.semaphore_signal(barrier, inc=1, device_id=peer, device_id_type=MESH_ID)
    cf_in = pltpu.make_async_copy(cf_hbm, cf, in_sem.at[0])
    leg_in = pltpu.make_async_copy(leg_hbm, leg, in_sem.at[1])
    pw_in = pltpu.make_async_copy(pw_hbm, pw, in_sem.at[2])
    cf_in.start()
    leg_in.start()
    pw_in.start()

    def slot_tile(ref, row, j):
        count = min(8, SLOTS - 8 * j)
        tile = ref[row, 8 * j : 8 * j + count, :].astype(F32)
        if count < 8:
            tile = jnp.concatenate([tile, jnp.zeros((8 - count, tile.shape[1]), F32)], 0)
        return tile

    cf_in.wait()
    for r in range(12):
        for g in range(2):
            tiles = [slot_tile(cf, r, 3 * g + k) for k in range(3)]
            at = 8 * (48 * g + 4 * r)
            for k in range(3):
                cbuf[at + 8 * k : at + 8 * k + 8, :] = tiles[k][:, :128]
            rest = [t[:, 128:] for t in tiles] + [jnp.zeros((8, 8), F32)]
            cbuf[at + 24 : at + 32, :] = jnp.concatenate(rest, 1)
    for g in range(2):
        for d in range(N):
            csend[g, d] = cbuf[pl.ds(384 * g + d, 48, stride=8), :].astype(BF)
    leg_in.wait()
    for i in range(LAT):
        for j in range(PER):
            at = 8 * (8 * j + i if i < 8 else 48 + 2 * j + i - 8)
            tile = slot_tile(leg, i, j)
            for l in range(6):
                lbuf[l, at : at + 8, :] = tile[:, 128 * l : 128 * l + 128]

    pl.semaphore_wait(barrier, len(peers))

    own_c = pltpu.make_async_copy(csend.at[:, z], crecv.at[:, z], own_sem.at[0])
    own_c.start()
    for g in range(2):
        for t in FAR_FIRST:
            to = (z + t) % N
            pltpu.make_async_remote_copy(
                csend.at[g, to], crecv.at[g, z], csem.at[0, g], csem.at[1, g],
                device_id=device(y, to, m), device_id_type=MESH_ID,
            ).start()

    pw_in.wait()

    @pl.loop(0, PER * N)
    def _(tile):
        first = SLOTS * (tile % N) + 8 * (tile // N)
        rows = [jnp.full((1, 128), pw[jnp.minimum(first + d, 359)].astype(F32)) for d in range(8)]
        ucol[pl.ds(pl.multiple_of(tile * 8, 8), 8), :] = jnp.concatenate(rows, 0)

    lane = lax.broadcasted_iota(jnp.int32, (16, 128), 1).astype(F32)

    def make_basis(first, last):
        @pl.loop(first, last)
        def _(block):
            at = pl.multiple_of(block * 16, 16)
            u = ucol[pl.ds(at, 16), :]
            odd = u - 2.0 * jnp.floor(u * 0.5) > 0.5
            even_wave = jnp.where(odd, float(DEG - 1) - u, u)
            weight = jnp.where(even_wave == 0.0, 1.0, 2.0)
            for h, (wave, wt) in enumerate(((even_wave, weight), (float(DEG - 1) - even_wave, 2.0))):
                for l in range(6):
                    pair = wave_rows(wave, wt, lane + 128.0 * l)
                    for e in range(2):
                        high, low = split_bf16(pair[e])
                        to = pl.multiple_of(384 * e + at, 16)
                        bas[h, 0, pl.ds(to, 16), 128 * l : 128 * l + 128] = high
                        bas[h, 1, pl.ds(to, 16), 128 * l : 128 * l + 128] = low

    make_basis(0, EARLY)

    def send_leg(to):
        pltpu.make_async_remote_copy(
            lsend.at[to], lrecv.at[z], lsem.at[0], lsem.at[1], device_id=device(y, to, m), device_id_type=MESH_ID
        ).start()

    for n, t in enumerate(FAR_FIRST + (0,)):
        to = (z + t) % N
        for l in range(6):
            lsend[to, :, 128 * l : 128 * l + 128] = lbuf[l, pl.ds(to, 60, stride=8), :].astype(BF)
        if n >= 1:
            send_leg((z + FAR_FIRST[n - 1]) % N)
    own_l = pltpu.make_async_copy(lsend.at[z], lrecv.at[z], own_sem.at[1])

    own_l.start()
    make_basis(EARLY, 24)

    def wait_bytes(ref, sem):
        pltpu.make_async_copy(ref, ref, sem).wait()

    def ring(way, step, half):
        origin = (y - step + N) % N if way == 0 else (y + step) % N
        part = gat.at[origin, pl.ds(4 * half, 4)]
        to = (y + 1) % N if way == 0 else (y + N - 1) % N
        return pltpu.make_async_remote_copy(
            part, part, ring_s.at[way, step, half], ring_r.at[way, step, half],
            device_id=device(to, z, m), device_id_type=MESH_ID,
        )

    own_c.wait()
    for half in range(2):
        wait_bytes(crecv.at[half, pl.ds(0, 7)], csem.at[1, half])
        for s in range(N):
            cbuf[48 * s : 48 * s + 48, :] = crecv[half, s].astype(F32)
        for blk in range(4):
            gat[y, 4 * half + blk] = cbuf[pl.ds(blk, 96, stride=4), :].astype(BF)
        for way in range(2):
            ring(way, 0, half).start()
    for step in range(1, 4):
        for half in range(2):
            for way in range(2):
                if step < 3 or way == half:
                    ring(way, step - 1, half).wait_recv()
                    ring(way, step, half).start()
    own_l.wait()
    wait_bytes(lrecv.at[pl.ds(0, 7)], lsem.at[1])
    for s in range(N):
        for l in range(6):
            ltail[l, 16 * s : 16 * s + 12, :] = lrecv[s, 48:60, 128 * l : 128 * l + 128].astype(F32)
    ring(0, 2, 1).wait_recv()
    ring(1, 2, 0).wait_recv()
    ring(0, 3, 0).wait_recv()
    ring(1, 3, 1).wait_recv()

    row_at = lax.broadcasted_iota(jnp.int32, (1, RR), 1)
    lane80 = lax.broadcasted_iota(jnp.int32, (80, 128), 1)
    for j in range(PER):
        u = pw[SLOTS * m + jnp.minimum(8 * j + z, SLOTS - 1)]
        cut = DEG - u
        odd = lax.rem(u, 2)
        low = (row_at < cut).astype(F32)
        high = (row_at <= DEG).astype(F32) - low
        swap = odd.astype(F32)
        masks = [(low + swap * (high - low)).astype(BF), (high + swap * (low - high)).astype(BF)]
        main = lrecv[:, 8 * j : 8 * j + 8, :].reshape(64, RR)
        tail = [[ltail[l, pl.ds(2 * j + k, 8, stride=16), :] for l in range(6)] for k in range(2)]
        tail = jnp.concatenate([jnp.concatenate(t, 1) for t in tail], 0)
        table = jnp.concatenate([main, tail.astype(BF)], 0)
        lhs = jnp.concatenate([table * masks[0], table * masks[1]], 0)
        g, k = divmod(j, 3)
        rhs = jnp.concatenate([gat[:, 4 * g + k].reshape(RR, 128), gat[:, 4 * g + 3].reshape(RR, 128)], 1)
        sums = jnp.dot(lhs, rhs, preferred_element_type=F32)
        for h in range(2):
            first = sums[80 * h : 80 * h + 80, :128]
            second = sums[80 * h : 80 * h + 80, 128:]
            imag = jnp.where(
                lane80 < 44, pltpu.roll(first, 44, axis=1), pltpu.roll(second, (44 - 40 * k) % 128, axis=1)
            )
            for e, value in enumerate((first, imag)):
                at = (12 * h + 6 * e + j) * STRIDE
                fbuf[at : at + 80, :] = jnp.where(lane80 < CH, value, 0.0)

    lane24 = lax.broadcasted_iota(jnp.int32, (24, 128), 1)

    def pack(to):
        lats = []
        for i in range(LAT):
            at = 8 * to + i if i < 8 else 64 + 8 * (i - 8) + to
            lats.append(fbuf[pl.ds(at, 24, stride=STRIDE), :])
        most = jnp.abs(lats[0])
        for value in lats[1:]:
            most = jnp.maximum(most, jnp.abs(value))
        most = jnp.max(most, axis=1, keepdims=True)
        level = jnp.ceil(jnp.log2(jnp.maximum(most, 1e-30)))
        gain = jnp.exp2(15.0 - level) * SHRINK
        lats = [jnp.round(value * gain) for value in lats]
        level = jnp.broadcast_to(level, (24, 128))
        for k in range(N):
            i, skip = k + k // 4, 21 * (k % 4)
            inside = (lane24 >= skip) & (lane24 < CH)
            window = jnp.where(inside, lats[i], pltpu.roll(lats[i + 1], CH, axis=1))
            window = jnp.where(lane24 == (skip + 127) % 128, level, window)
            fsend[to, k] = window.astype(jnp.int32).astype(jnp.int16)

    def send_f(to):
        for t in range(N):
            m_to = (m + t) % N
            pltpu.make_async_remote_copy(
                fsend.at[to, m_to], frecv.at[m * N + z], fsem.at[0], fsem.at[1],
                device_id=device(y, to, m_to), device_id_type=MESH_ID,
            ).start()

    for n, t in enumerate(FAR_FIRST + (0,)):
        pack((z + t) % N)
        if n >= 1:
            send_f((z + FAR_FIRST[n - 1]) % N)
    for t in range(1, N):
        m_to = (m + t) % N
        pltpu.make_async_remote_copy(
            fsend.at[z, m_to], frecv.at[m * N + z], fsem.at[0], fsem.at[1],
            device_id=device(y, z, m_to), device_id_type=MESH_ID,
        ).start()
    own_f = pltpu.make_async_copy(fsend.at[z, m], frecv.at[m * N + z], own_sem.at[2])
    own_f.start()

    for g in range(2):
        wait_bytes(csend.at[g, pl.ds(0, 7)], csem.at[0, g])
    wait_bytes(lsend.at[pl.ds(0, 7)], lsem.at[0])
    for way in range(2):
        for step in range(4):
            for half in range(2):
                if step < 3 or way == half:
                    ring(way, step, half).wait_send()
    own_f.wait()
    wait_bytes(frecv.at[pl.ds(0, 63)], fsem.at[1])

    turn = lax.rem(128 - 21 * lax.rem(m, 4), 128)

    @pl.loop(0, 8)
    def _(part):
        coded = frecv[pl.ds(part * 8, 8)].astype(jnp.int32).astype(F32).reshape(192, 128)
        fdec[pl.ds(pl.multiple_of(part * 192, 8), 192), :] = pltpu.roll(coded, turn, axis=1)

    lhs = []
    for h in range(2):
        rows = jnp.concatenate([fdec[pl.ds(12 * h + t, 64, stride=24), :] for t in range(12)], 0)
        rows = jnp.transpose(rows)
        rows = rows * (jnp.exp2(rows[127:128, :] - 15.0) * (1.0 / SHRINK))
        high, low = split_bf16(rows)
        lhs.append((high, jnp.concatenate([high, low], 0)))
    for l in range(3):
        at = slice(256 * l, 256 * l + 256)
        part = []
        for h in range(2):
            high, both = lhs[h]
            wide = jnp.dot(both, bas[h, 0, :, at], preferred_element_type=F32)
            part.append(
                wide[:128] + wide[128:] + jnp.dot(high, bas[h, 1, :, at], preferred_element_type=F32)
            )
        count = min(256, HALF - 256 * l)
        out[:, 256 * l : 256 * l + count] = (part[0] + part[1])[:ROWS, :count]
        out[:, HALF + 256 * l : HALF + 256 * l + count] = (part[0] - part[1])[:ROWS, :count]
    wait_bytes(frecv.at[pl.ds(0, 63)], fsem.at[0])


def body(pair_wave, legendre, coefs):
    i16 = jnp.int16
    return pl.pallas_call(
        kernel,
        out_shape=jax.ShapeDtypeStruct((ROWS, LON), F32),
        in_specs=[
            pl.BlockSpec(memory_space=pltpu.HBM),
            pl.BlockSpec(memory_space=pltpu.HBM),
            pl.BlockSpec(memory_space=pltpu.HBM),
        ],
        out_specs=pl.BlockSpec(memory_space=pltpu.VMEM),
        scratch_shapes=[
            pltpu.SMEM((360,), jnp.int32),
            pltpu.VMEM((LAT, SLOTS, RR), BF),
            pltpu.VMEM((12, SLOTS, 2 * CH), BF),
            pltpu.VMEM((768, 128), F32),
            pltpu.VMEM((2, N, 48, 128), BF),
            pltpu.VMEM((2, N, 48, 128), BF),
            pltpu.VMEM((N, 8, 96, 128), BF),
            pltpu.VMEM((6, 480, 128), F32),
            pltpu.VMEM((N, 60, RR), BF),
            pltpu.VMEM((N, 60, RR), BF),
            pltpu.VMEM((6, 128, 128), F32),
            pltpu.VMEM((24 * STRIDE, 128), F32),
            pltpu.VMEM((N, N, 24, 128), i16),
            pltpu.VMEM((N * N, 24, 128), i16),
            pltpu.VMEM((N * N * 24, 128), F32),
            pltpu.VMEM((384, 128), F32),
            pltpu.VMEM((2, 2, RR, RR), BF),
            pltpu.SemaphoreType.DMA((3,)),
            pltpu.SemaphoreType.DMA((3,)),
            pltpu.SemaphoreType.DMA((2, 2)),
            pltpu.SemaphoreType.DMA((2,)),
            pltpu.SemaphoreType.DMA((2,)),
            pltpu.SemaphoreType.DMA((2, 4, 2)),
            pltpu.SemaphoreType.DMA((2, 4, 2)),
        ],
        compiler_params=pltpu.CompilerParams(collective_id=0, has_side_effects=True, vmem_limit_bytes=67043328),
    )(pair_wave, jnp.transpose(legendre, (1, 0, 2)), jnp.transpose(coefs, (1, 0, 2)))


def solution(mesh):
    split = Mesh(mesh.devices.reshape(N, N, 4, 2), ("y", "z", "x", "c"))
    placed = (P(), P(("x", "c"), ("y", "z"), None), P(("x", "c"), ("y", "z"), None))
    return jax.shard_map(
        body, mesh=split, in_specs=placed, out_specs=P(("y", "z", "x", "c"), None), check_vma=False
    )
```

```python
import math

import jax
import jax.numpy as jnp
import numpy as np
from jax import lax
from jax.experimental import pallas as pl
from jax.experimental.pallas import tpu as pltpu
from jax.sharding import Mesh
from jax.sharding import PartitionSpec as P

DEG = 720
LON = 1440
HALF = LON // 2
CH = 84
LAT = 10
SLOTS = 45
PER = 6
N = 8
ROWS = 105
RR = 768
F32 = jnp.float32
BF = jnp.bfloat16
MESH_ID = pl.DeviceIdType.MESH
FAR_FIRST = (4, 3, 5, 2, 6, 1, 7)
STRIDE = 88
BEFORE = (4, 3, 5)
BETWEEN = ((2, 6), (1, 7), ())
EARLY = 8
LATER = 8
SHRINK = 0.9999


def half_angle_fit():
    t = np.cos(np.linspace(0, np.pi, 4001)) * (np.pi / 2)
    sin_c = np.linalg.lstsq(np.stack([t ** (2 * i + 1) for i in range(5)], 1), np.sin(t), rcond=None)[0]
    cos_c = np.linalg.lstsq(np.stack([t ** (2 * i) for i in range(6)], 1), np.cos(t), rcond=None)[0]
    return [float(v) for v in sin_c], [float(v) for v in cos_c]


SIN_C, COS_C = half_angle_fit()


def horner(coefs, square):
    total = jnp.full_like(square, coefs[-1])
    for value in coefs[-2::-1]:
        total = total * square + value
    return total


def wave_rows(waves, weight, lon_at):
    product = waves * lon_at
    turns = jnp.round(product * (1.0 / LON))
    half = (product - turns * float(LON)) * (math.pi / LON)
    square = half * half
    sine = half * horner(SIN_C, square)
    cosine = horner(COS_C, square)
    twice = (2.0 * weight) * sine
    return weight - twice * sine, -twice * cosine


def split_bf16(x):
    high = x.astype(BF)
    return high, (x - high.astype(F32)).astype(BF)


def natural_rows():
    lane = lax.broadcasted_iota(jnp.int32, (1, RR), 1).astype(F32)
    z_at = jnp.floor((lane + 0.5) * (1.0 / 96))
    rest = lane - 96.0 * z_at
    y_at = jnp.floor((rest + 0.5) * (1.0 / 12))
    return lane, (8.0 * y_at + z_at) * 12.0 + rest - 12.0 * y_at


def kernel(
    pw_hbm, leg_hbm, cf_hbm, out,
    pw, leg, cf, perm, cbuf, csend, crecv, gat, lbuf, lsend, lrecv, ltail, fbuf, fsend, frecv, fdec, ucol, bas,
    in_sem, own_sem, csem, lsem, fsem, ring_s, ring_r,
):
    y, z = lax.axis_index("y"), lax.axis_index("z")
    m = 2 * lax.axis_index("x") + lax.axis_index("c")
    along, across = (z, y), (y, z)

    def device(kind, along_at, across_at, m_at):
        place = (across_at, along_at) if kind == 0 else (along_at, across_at)
        return (*place, m_at // 2, m_at % 2)

    barrier = pltpu.get_barrier_semaphore()
    peers = [device(kind, (along[kind] + t) % N, across[kind], m) for t in FAR_FIRST for kind in range(2)]
    peers += [device(0, z, y, (m + t) % N) for t in FAR_FIRST]
    for peer in peers:
        pl.semaphore_signal(barrier, inc=1, device_id=peer, device_id_type=MESH_ID)
    cf_in = pltpu.make_async_copy(cf_hbm, cf, in_sem.at[0])
    leg_in = pltpu.make_async_copy(leg_hbm, leg, in_sem.at[1])
    pw_in = pltpu.make_async_copy(pw_hbm, pw, in_sem.at[2])
    cf_in.start()
    leg_in.start()
    pw_in.start()

    lane_row, natural = natural_rows()

    @pl.loop(0, 48)
    def _(block):
        row = lax.broadcasted_iota(jnp.int32, (16, RR), 0).astype(F32) + (16 * block).astype(F32)
        perm[pl.ds(pl.multiple_of(block * 16, 16), 16), :] = jnp.where(row == natural, 1.0, 0.0).astype(BF)

    def slot_tile(ref, row, j):
        count = min(8, SLOTS - 8 * j)
        tile = ref[row, 8 * j : 8 * j + count, :].astype(F32)
        if count < 8:
            tile = jnp.concatenate([tile, jnp.zeros((8 - count, tile.shape[1]), F32)], 0)
        return tile

    cf_in.wait()
    for r in range(12):
        for g in range(2):
            tiles = [slot_tile(cf, r, 3 * g + k) for k in range(3)]
            at = 8 * (48 * g + 4 * r)
            for k in range(3):
                cbuf[at + 8 * k : at + 8 * k + 8, :] = tiles[k][:, :128]
            rest = [t[:, 128:] for t in tiles] + [jnp.zeros((8, 8), F32)]
            cbuf[at + 24 : at + 32, :] = jnp.concatenate(rest, 1)
    for g in range(2):
        for d in range(N):
            csend[g, d] = cbuf[pl.ds(384 * g + d, 48, stride=8), :].astype(BF)

    def put_leg(kind, i, k, tile):
        at = 240 * kind + 8 * (8 * k + i if i < 8 else 24 + 2 * k + i - 8)
        for l in range(6):
            lbuf[l, at : at + 8, :] = tile[:, 128 * l : 128 * l + 128]

    def pack_leg(kind):
        for d in range(N):
            for l in range(6):
                rows = lbuf[l, pl.ds(240 * kind + d, 30, stride=8), :]
                lsend[kind, d, :, 128 * l : 128 * l + 128] = rows.astype(BF)

    leg_in.wait()
    for i in range(LAT):
        for k in range(3):
            put_leg(0, i, k, slot_tile(leg, i, k))
    pack_leg(0)

    pl.semaphore_wait(barrier, len(peers))

    own_c = pltpu.make_async_copy(
        csend.at[0, along[0]], crecv.at[0, along[0]], own_sem.at[0]
    ), pltpu.make_async_copy(csend.at[1, along[1]], crecv.at[1, along[1]], own_sem.at[1])
    for t in FAR_FIRST:
        for kind in range(2):
            to = (along[kind] + t) % N
            pltpu.make_async_remote_copy(
                csend.at[kind, to], crecv.at[kind, along[kind]], csem.at[0, kind], csem.at[1, kind],
                device_id=device(kind, to, across[kind], m), device_id_type=MESH_ID,
            ).start()
    own_c[0].start()
    own_c[1].start()

    def send_leg(t):
        for kind in range(2):
            to = (along[kind] + t) % N
            pltpu.make_async_remote_copy(
                lsend.at[kind, to], lrecv.at[kind, t], lsem.at[0, kind], lsem.at[1, kind],
                device_id=device(kind, to, across[kind], m), device_id_type=MESH_ID,
            ).start()

    rows = [jnp.concatenate([slot_tile(leg, i, 3 + k) for k in range(3)], 0).astype(BF) for i in range(LAT)]
    moved = jnp.dot(jnp.concatenate(rows, 0), perm[...], preferred_element_type=F32)
    for i in range(LAT):
        for k in range(3):
            put_leg(1, i, k, moved[24 * i + 8 * k : 24 * i + 8 * k + 8])
    pack_leg(1)
    pw_in.wait()

    @pl.loop(0, PER * N)
    def _(tile):
        first = SLOTS * (tile % N) + 8 * (tile // N)
        rows = [jnp.full((1, 128), pw[jnp.minimum(first + d, 359)].astype(F32)) for d in range(8)]
        ucol[pl.ds(pl.multiple_of(tile * 8, 8), 8), :] = jnp.concatenate(rows, 0)

    lane = lax.broadcasted_iota(jnp.int32, (16, 128), 1).astype(F32)

    def make_basis(first, last):
        @pl.loop(first, last)
        def _(block):
            at = pl.multiple_of(block * 16, 16)
            u = ucol[pl.ds(at, 16), :]
            odd = u - 2.0 * jnp.floor(u * 0.5) > 0.5
            even_wave = jnp.where(odd, float(DEG - 1) - u, u)
            weight = jnp.where(even_wave == 0.0, 1.0, 2.0)
            for h, (wave, wt) in enumerate(((even_wave, weight), (float(DEG - 1) - even_wave, 2.0))):
                for l in range(6):
                    pair = wave_rows(wave, wt, lane + 128.0 * l)
                    for e in range(2):
                        high, low = split_bf16(pair[e])
                        to = pl.multiple_of(384 * e + at, 16)
                        bas[h, 0, pl.ds(to, 16), 128 * l : 128 * l + 128] = high
                        bas[h, 1, pl.ds(to, 16), 128 * l : 128 * l + 128] = low

    own_l = [
        pltpu.make_async_copy(lsend.at[kind, along[kind]], lrecv.at[kind, 0], own_sem.at[2 + kind])
        for kind in range(2)
    ]
    for t in BEFORE:
        send_leg(t)
    own_l[0].start()
    own_l[1].start()
    make_basis(0, EARLY)

    def wait_bytes(ref, sem):
        pltpu.make_async_copy(ref, ref, sem).wait()

    def ring(kind, way, step, half):
        own = across[kind]
        origin = (own - step + N) % N if way == 0 else (own + step) % N
        part = gat.at[kind, origin, pl.ds(2 * half, 2)]
        to = (own + 1) % N if way == 0 else (own + N - 1) % N
        return pltpu.make_async_remote_copy(
            part, part, ring_s.at[kind, way, step, half], ring_r.at[kind, way, step, half],
            device_id=device(kind, along[kind], to, m), device_id_type=MESH_ID,
        )

    for kind in range(2):
        own_c[kind].wait()
        wait_bytes(crecv.at[kind, pl.ds(0, 7)], csem.at[1, kind])
        for s in range(N):
            cbuf[48 * s : 48 * s + 48, :] = crecv[kind, s].astype(F32)
        for blk in range(4):
            gat[kind, across[kind], blk] = cbuf[pl.ds(blk, 96, stride=4), :].astype(BF)
        for half in range(2):
            for way in range(2):
                ring(kind, way, 0, half).start()
    for step in range(1, 4):
        for t in BETWEEN[step - 1]:
            send_leg(t)
        if step < 3:
            make_basis(EARLY + LATER * (step - 1), min(24, EARLY + LATER * step))
        for half in range(2):
            for kind in range(2):
                for way in range(2):
                    if step < 3 or way == half:
                        ring(kind, way, step - 1, half).wait_recv()
                        ring(kind, way, step, half).start()
    for kind in range(2):
        own_l[kind].wait()
        wait_bytes(lrecv.at[kind, pl.ds(0, 7)], lsem.at[1, kind])
        for t in range(N):
            for l in range(6):
                ltail[kind, l, 8 * t : 8 * t + 6, :] = lrecv[kind, t, 24:30, 128 * l : 128 * l + 128].astype(F32)
    for kind in range(2):
        ring(kind, 0, 2, 1).wait_recv()
        ring(kind, 1, 2, 0).wait_recv()
        ring(kind, 0, 3, 0).wait_recv()
        ring(kind, 1, 3, 1).wait_recv()

    lane80 = lax.broadcasted_iota(jnp.int32, (80, 128), 1)
    for j in range(PER):
        kind, k = divmod(j, 3)
        u = pw[SLOTS * m + jnp.minimum(8 * j + along[kind], SLOTS - 1)]
        row_at = natural if kind else lane_row
        low = (row_at < (DEG - u).astype(F32)).astype(F32)
        high = (row_at <= float(DEG)).astype(F32) - low
        swap = lax.rem(u, 2).astype(F32)
        masks = [(low + swap * (high - low)).astype(BF), (high + swap * (low - high)).astype(BF)]
        main = lrecv[kind, :, 8 * k : 8 * k + 8, :].reshape(64, RR)
        tail = [[ltail[kind, l, pl.ds(2 * k + n, 8, stride=8), :] for l in range(6)] for n in range(2)]
        tail = jnp.concatenate([jnp.concatenate(t, 1) for t in tail], 0)
        table = jnp.concatenate([main, tail.astype(BF)], 0)
        lhs = jnp.concatenate([table * masks[0], table * masks[1]], 0)
        rhs = jnp.concatenate([gat[kind, :, k].reshape(RR, 128), gat[kind, :, 3].reshape(RR, 128)], 1)
        sums = jnp.dot(lhs, rhs, preferred_element_type=F32)
        for h in range(2):
            first = sums[80 * h : 80 * h + 80, :128]
            second = sums[80 * h : 80 * h + 80, 128:]
            imag = jnp.where(
                lane80 < 44, pltpu.roll(first, 44, axis=1), pltpu.roll(second, (44 - 40 * k) % 128, axis=1)
            )
            for e, value in enumerate((first, imag)):
                n = 6 * h + 3 * e + k
                at = (8 * kind + n if n < 8 else 16 + 4 * kind + n - 8) * STRIDE
                fbuf[at : at + 80, :] = jnp.where(lane80 < CH, value, 0.0)

    lane24 = lax.broadcasted_iota(jnp.int32, (24, 128), 1)

    def pack(t):
        lats = []
        for i in range(LAT):
            at = 8 * t + i if i < 8 else 64 + 8 * (i - 8) + t
            lats.append(fbuf[pl.ds(at, 24, stride=STRIDE), :])
        most = jnp.abs(lats[0])
        for value in lats[1:]:
            most = jnp.maximum(most, jnp.abs(value))
        most = jnp.max(most, axis=1, keepdims=True)
        level = jnp.ceil(jnp.log2(jnp.maximum(most, 1e-30)))
        gain = jnp.exp2(15.0 - level) * SHRINK
        lats = [jnp.round(value * gain) for value in lats]
        level = jnp.broadcast_to(level, (24, 128))
        for k in range(N):
            i, skip = k + k // 4, 21 * (k % 4)
            inside = (lane24 >= skip) & (lane24 < CH)
            window = jnp.where(inside, lats[i], pltpu.roll(lats[i + 1], CH, axis=1))
            window = jnp.where(lane24 == (skip + 127) % 128, level, window).astype(jnp.int32)
            for kind in range(2):
                fsend[t, k, kind, 0:8] = window[8 * kind : 8 * kind + 8].astype(jnp.int16)
                fsend[t, k, kind, 8:12] = window[16 + 4 * kind : 20 + 4 * kind].astype(jnp.int16)

    def send_f(t):
        for n in range(0 if t else 1, N):
            m_to = (m + n) % N
            for kind in range(2):
                to = (along[kind] - t + N) % N
                pltpu.make_async_remote_copy(
                    fsend.at[t, m_to, kind], frecv.at[kind, m * N + along[kind]], fsem.at[0, kind], fsem.at[1, kind],
                    device_id=device(kind, to, across[kind], m_to), device_id_type=MESH_ID,
                ).start()

    order = FAR_FIRST + (0,)
    for n, t in enumerate(order):
        pack(t)
        if n >= 1:
            send_f(order[n - 1])
    send_f(0)
    own_f = [
        pltpu.make_async_copy(fsend.at[0, m, kind], frecv.at[kind, m * N + along[kind]], own_sem.at[4 + kind])
        for kind in range(2)
    ]
    own_f[0].start()
    own_f[1].start()

    for kind in range(2):
        wait_bytes(csend.at[kind, pl.ds(0, 7)], csem.at[0, kind])
        wait_bytes(lsend.at[kind, pl.ds(0, 7)], lsem.at[0, kind])
        for way in range(2):
            for step in range(4):
                for half in range(2):
                    if step < 3 or way == half:
                        ring(kind, way, step, half).wait_send()

    turn = lax.rem(128 - 21 * lax.rem(m, 4), 128)
    for kind in range(2):
        own_f[kind].wait()
        wait_bytes(frecv.at[kind, pl.ds(0, 63)], fsem.at[1, kind])

        @pl.loop(0, 8)
        def _(part):
            coded = frecv[kind, pl.ds(part * 8, 8)].astype(jnp.int32).astype(F32)
            for n in range(8):
                at = pl.multiple_of((64 * kind + part * 8 + n) * 24, 8)
                fdec[pl.ds(at, 12), :] = pltpu.roll(coded[n], turn, axis=1)

    lhs = []
    for h in range(2):
        at = [1536 * kind + 6 * h + 3 * e + k for e in range(2) for kind in range(2) for k in range(3)]
        rows = jnp.concatenate([fdec[pl.ds(first, 64, stride=24), :] for first in at], 0)
        rows = jnp.transpose(rows)
        rows = rows * (jnp.exp2(rows[127:128, :] - 15.0) * (1.0 / SHRINK))
        high, low = split_bf16(rows)
        lhs.append((high, jnp.concatenate([high, low], 0)))
    for l in range(3):
        at = slice(256 * l, 256 * l + 256)
        part = []
        for h in range(2):
            high, both = lhs[h]
            wide = jnp.dot(both, bas[h, 0, :, at], preferred_element_type=F32)
            part.append(
                wide[:128] + wide[128:] + jnp.dot(high, bas[h, 1, :, at], preferred_element_type=F32)
            )
        count = min(256, HALF - 256 * l)
        out[:, 256 * l : 256 * l + count] = (part[0] + part[1])[:ROWS, :count]
        out[:, HALF + 256 * l : HALF + 256 * l + count] = (part[0] - part[1])[:ROWS, :count]
    for kind in range(2):
        wait_bytes(frecv.at[kind, pl.ds(0, 63)], fsem.at[0, kind])


def body(pair_wave, legendre, coefs):
    i16 = jnp.int16
    return pl.pallas_call(
        kernel,
        out_shape=jax.ShapeDtypeStruct((ROWS, LON), F32),
        in_specs=[
            pl.BlockSpec(memory_space=pltpu.HBM),
            pl.BlockSpec(memory_space=pltpu.HBM),
            pl.BlockSpec(memory_space=pltpu.HBM),
        ],
        out_specs=pl.BlockSpec(memory_space=pltpu.VMEM),
        scratch_shapes=[
            pltpu.SMEM((360,), jnp.int32),
            pltpu.VMEM((LAT, SLOTS, RR), BF),
            pltpu.VMEM((12, SLOTS, 2 * CH), BF),
            pltpu.VMEM((RR, RR), BF),
            pltpu.VMEM((768, 128), F32),
            pltpu.VMEM((2, N, 48, 128), BF),
            pltpu.VMEM((2, N, 48, 128), BF),
            pltpu.VMEM((2, N, 4, 96, 128), BF),
            pltpu.VMEM((6, 480, 128), F32),
            pltpu.VMEM((2, N, 30, RR), BF),
            pltpu.VMEM((2, N, 30, RR), BF),
            pltpu.VMEM((2, 6, 64, 128), F32),
            pltpu.VMEM((24 * STRIDE, 128), F32),
            pltpu.VMEM((N, N, 2, 12, 128), i16),
            pltpu.VMEM((2, N * N, 12, 128), i16),
            pltpu.VMEM((2 * N * N * 24, 128), F32),
            pltpu.VMEM((384, 128), F32),
            pltpu.VMEM((2, 2, RR, RR), BF),
            pltpu.SemaphoreType.DMA((3,)),
            pltpu.SemaphoreType.DMA((6,)),
            pltpu.SemaphoreType.DMA((2, 2)),
            pltpu.SemaphoreType.DMA((2, 2)),
            pltpu.SemaphoreType.DMA((2, 2)),
            pltpu.SemaphoreType.DMA((2, 2, 4, 2)),
            pltpu.SemaphoreType.DMA((2, 2, 4, 2)),
        ],
        compiler_params=pltpu.CompilerParams(collective_id=0, has_side_effects=True, vmem_limit_bytes=67043328),
    )(pair_wave, jnp.transpose(legendre, (1, 0, 2)), jnp.transpose(coefs, (1, 0, 2)))


def solution(mesh):
    split = Mesh(mesh.devices.reshape(N, N, 4, 2), ("y", "z", "x", "c"))
    placed = (P(), P(("x", "c"), ("y", "z"), None), P(("x", "c"), ("y", "z"), None))
    return jax.shard_map(
        body, mesh=split, in_specs=placed, out_specs=P(("y", "z", "x", "c"), None), check_vma=False
    )
```

```python
import math

import jax
import jax.numpy as jnp
import numpy as np
from jax import lax
from jax.experimental import pallas as pl
from jax.experimental.pallas import tpu as pltpu
from jax.sharding import Mesh
from jax.sharding import PartitionSpec as P

DEG = 720
LON = 1440
HALF = LON // 2
CH = 84
LAT = 10
SLOTS = 45
PER = 6
N = 8
ROWS = 105
RR = 768
F32 = jnp.float32
BF = jnp.bfloat16
MESH_ID = pl.DeviceIdType.MESH
FAR_FIRST = (4, 3, 5, 2, 6, 1, 7)
STRIDE = 88
BEFORE = (4, 3, 5)
BETWEEN = ((2, 6), (1, 7))
EARLY = 8
LATER = 8
SHRINK = 0.9999


def half_angle_fit():
    t = np.cos(np.linspace(0, np.pi, 4001)) * (np.pi / 2)
    sin_c = np.linalg.lstsq(np.stack([t ** (2 * i + 1) for i in range(5)], 1), np.sin(t), rcond=None)[0]
    cos_c = np.linalg.lstsq(np.stack([t ** (2 * i) for i in range(6)], 1), np.cos(t), rcond=None)[0]
    return [float(v) for v in sin_c], [float(v) for v in cos_c]


SIN_C, COS_C = half_angle_fit()


def horner(coefs, square):
    total = jnp.full_like(square, coefs[-1])
    for value in coefs[-2::-1]:
        total = total * square + value
    return total


def wave_rows(waves, weight, lon_at):
    product = waves * lon_at
    turns = jnp.round(product * (1.0 / LON))
    half = (product - turns * float(LON)) * (math.pi / LON)
    square = half * half
    sine = half * horner(SIN_C, square)
    cosine = horner(COS_C, square)
    twice = (2.0 * weight) * sine
    return weight - twice * sine, -twice * cosine


def split_bf16(x):
    high = x.astype(BF)
    return high, (x - high.astype(F32)).astype(BF)


def natural_rows():
    lane = lax.broadcasted_iota(jnp.int32, (1, RR), 1).astype(F32)
    z_at = jnp.floor((lane + 0.5) * (1.0 / 96))
    rest = lane - 96.0 * z_at
    y_at = jnp.floor((rest + 0.5) * (1.0 / 12))
    return lane, (8.0 * y_at + z_at) * 12.0 + rest - 12.0 * y_at


def kernel(
    pw_hbm, leg_hbm, cf_hbm, out,
    pw, leg, cf, perm, cbuf, csend, crecv, gat, lbuf, lsend, lrecv, ltail, fbuf, fsend, frecv, fdec, ucol, bas,
    in_sem, own_sem, csem, lsem, fsem, ring_s, ring_r,
):
    y, z = lax.axis_index("y"), lax.axis_index("z")
    m = 2 * lax.axis_index("x") + lax.axis_index("c")
    along, across = (z, y), (y, z)

    def device(kind, along_at, across_at, m_at):
        place = (across_at, along_at) if kind == 0 else (along_at, across_at)
        return (*place, m_at // 2, m_at % 2)

    barrier = pltpu.get_barrier_semaphore()
    peers = [device(kind, (along[kind] + t) % N, across[kind], m) for t in FAR_FIRST for kind in range(2)]
    peers += [device(0, z, y, (m + t) % N) for t in FAR_FIRST]
    for peer in peers:
        pl.semaphore_signal(barrier, inc=1, device_id=peer, device_id_type=MESH_ID)
    cf_in = pltpu.make_async_copy(cf_hbm, cf, in_sem.at[0])
    leg_in = pltpu.make_async_copy(leg_hbm, leg, in_sem.at[1])
    pw_in = pltpu.make_async_copy(pw_hbm, pw, in_sem.at[2])
    cf_in.start()
    leg_in.start()
    pw_in.start()

    lane_row, natural = natural_rows()

    @pl.loop(0, 48)
    def _(block):
        row = lax.broadcasted_iota(jnp.int32, (16, RR), 0).astype(F32) + (16 * block).astype(F32)
        perm[pl.ds(pl.multiple_of(block * 16, 16), 16), :] = jnp.where(row == natural, 1.0, 0.0).astype(BF)

    def slot_tile(ref, row, j):
        count = min(8, SLOTS - 8 * j)
        tile = ref[row, 8 * j : 8 * j + count, :].astype(F32)
        if count < 8:
            tile = jnp.concatenate([tile, jnp.zeros((8 - count, tile.shape[1]), F32)], 0)
        return tile

    cf_in.wait()
    for r in range(12):
        for g in range(2):
            tiles = [slot_tile(cf, r, 3 * g + k) for k in range(3)]
            at = 8 * (48 * g + 4 * r)
            for k in range(3):
                cbuf[at + 8 * k : at + 8 * k + 8, :] = tiles[k][:, :128]
            rest = [t[:, 128:] for t in tiles] + [jnp.zeros((8, 8), F32)]
            cbuf[at + 24 : at + 32, :] = jnp.concatenate(rest, 1)
    for g in range(2):
        for d in range(N):
            csend[g, d] = cbuf[pl.ds(384 * g + d, 48, stride=8), :].astype(BF)

    def put_leg(kind, i, k, tile):
        at = 240 * kind + 8 * (8 * k + i if i < 8 else 24 + 2 * k + i - 8)
        for l in range(6):
            lbuf[l, at : at + 8, :] = tile[:, 128 * l : 128 * l + 128]

    def pack_leg(kind):
        for d in range(N):
            for l in range(6):
                rows = lbuf[l, pl.ds(240 * kind + d, 30, stride=8), :]
                lsend[kind, d, :, 128 * l : 128 * l + 128] = rows.astype(BF)

    leg_in.wait()
    for i in range(LAT):
        for k in range(3):
            put_leg(0, i, k, slot_tile(leg, i, k))
    pack_leg(0)

    pl.semaphore_wait(barrier, len(peers))

    own_c = pltpu.make_async_copy(
        csend.at[0, along[0]], crecv.at[0, along[0]], own_sem.at[0]
    ), pltpu.make_async_copy(csend.at[1, along[1]], crecv.at[1, along[1]], own_sem.at[1])
    for t in FAR_FIRST:
        for kind in range(2):
            to = (along[kind] + t) % N
            pltpu.make_async_remote_copy(
                csend.at[kind, to], crecv.at[kind, along[kind]], csem.at[0, kind], csem.at[1, kind],
                device_id=device(kind, to, across[kind], m), device_id_type=MESH_ID,
            ).start()
    own_c[0].start()
    own_c[1].start()

    def send_leg(t):
        for kind in range(2):
            to = (along[kind] + t) % N
            pltpu.make_async_remote_copy(
                lsend.at[kind, to], lrecv.at[kind, t], lsem.at[0, kind], lsem.at[1, kind],
                device_id=device(kind, to, across[kind], m), device_id_type=MESH_ID,
            ).start()

    rows = [jnp.concatenate([slot_tile(leg, i, 3 + k) for k in range(3)], 0).astype(BF) for i in range(LAT)]
    moved = jnp.dot(jnp.concatenate(rows, 0), perm[...], preferred_element_type=F32)
    for i in range(LAT):
        for k in range(3):
            put_leg(1, i, k, moved[24 * i + 8 * k : 24 * i + 8 * k + 8])
    pack_leg(1)
    for t in BEFORE:
        send_leg(t)
    pw_in.wait()

    @pl.loop(0, PER * N)
    def _(tile):
        first = SLOTS * (tile % N) + 8 * (tile // N)
        rows = [jnp.full((1, 128), pw[jnp.minimum(first + d, 359)].astype(F32)) for d in range(8)]
        ucol[pl.ds(pl.multiple_of(tile * 8, 8), 8), :] = jnp.concatenate(rows, 0)

    lane = lax.broadcasted_iota(jnp.int32, (16, 128), 1).astype(F32)

    def make_basis(first, last):
        @pl.loop(first, last)
        def _(block):
            at = pl.multiple_of(block * 16, 16)
            u = ucol[pl.ds(at, 16), :]
            odd = u - 2.0 * jnp.floor(u * 0.5) > 0.5
            even_wave = jnp.where(odd, float(DEG - 1) - u, u)
            weight = jnp.where(even_wave == 0.0, 1.0, 2.0)
            for h, (wave, wt) in enumerate(((even_wave, weight), (float(DEG - 1) - even_wave, 2.0))):
                for l in range(6):
                    pair = wave_rows(wave, wt, lane + 128.0 * l)
                    for e in range(2):
                        high, low = split_bf16(pair[e])
                        to = pl.multiple_of(384 * e + at, 16)
                        bas[h, 0, pl.ds(to, 16), 128 * l : 128 * l + 128] = high
                        bas[h, 1, pl.ds(to, 16), 128 * l : 128 * l + 128] = low

    own_l = [
        pltpu.make_async_copy(lsend.at[kind, along[kind]], lrecv.at[kind, 0], own_sem.at[2 + kind])
        for kind in range(2)
    ]
    own_l[0].start()
    own_l[1].start()
    make_basis(0, EARLY)

    def wait_bytes(ref, sem):
        pltpu.make_async_copy(ref, ref, sem).wait()

    def ring(kind, way, step, half):
        own, back, on = across[kind], min(step, 2), 1 + step // 3
        origin = (own - back + N) % N if way == 0 else (own + back) % N
        part = gat.at[kind, origin, pl.ds(2 * half, 2)]
        to = (own + on) % N if way == 0 else (own + N - on) % N
        return pltpu.make_async_remote_copy(
            part, part, ring_s.at[kind, way, step, half], ring_r.at[kind, way, step, half],
            device_id=device(kind, along[kind], to, m), device_id_type=MESH_ID,
        )

    for kind in range(2):
        own_c[kind].wait()
        wait_bytes(crecv.at[kind, pl.ds(0, 7)], csem.at[1, kind])
        for s in range(N):
            cbuf[48 * s : 48 * s + 48, :] = crecv[kind, s].astype(F32)
        for blk in range(4):
            gat[kind, across[kind], blk] = cbuf[pl.ds(blk, 96, stride=4), :].astype(BF)
        for half in range(2):
            for way in range(2):
                ring(kind, way, 0, half).start()
    for step in range(1, 3):
        for t in BETWEEN[step - 1]:
            send_leg(t)
        make_basis(EARLY + LATER * (step - 1), min(24, EARLY + LATER * step))
        for half in range(2):
            for kind in range(2):
                for way in range(2):
                    ring(kind, way, step - 1, half).wait_recv()
                    if step == 2 and way == half:
                        ring(kind, way, 3, half).start()
                    ring(kind, way, step, half).start()
    for kind in range(2):
        own_l[kind].wait()
        wait_bytes(lrecv.at[kind, pl.ds(0, 7)], lsem.at[1, kind])
        for t in range(N):
            for l in range(6):
                ltail[kind, l, 8 * t : 8 * t + 6, :] = lrecv[kind, t, 24:30, 128 * l : 128 * l + 128].astype(F32)
    for kind in range(2):
        for way in range(2):
            for half in range(2):
                ring(kind, way, 2, half).wait_recv()
            ring(kind, way, 3, way).wait_recv()

    lane80 = lax.broadcasted_iota(jnp.int32, (80, 128), 1)
    for j in range(PER):
        kind, k = divmod(j, 3)
        u = pw[SLOTS * m + jnp.minimum(8 * j + along[kind], SLOTS - 1)]
        row_at = natural if kind else lane_row
        low = (row_at < (DEG - u).astype(F32)).astype(F32)
        high = (row_at <= float(DEG)).astype(F32) - low
        swap = lax.rem(u, 2).astype(F32)
        masks = [(low + swap * (high - low)).astype(BF), (high + swap * (low - high)).astype(BF)]
        main = lrecv[kind, :, 8 * k : 8 * k + 8, :].reshape(64, RR)
        tail = [[ltail[kind, l, pl.ds(2 * k + n, 8, stride=8), :] for l in range(6)] for n in range(2)]
        tail = jnp.concatenate([jnp.concatenate(t, 1) for t in tail], 0)
        table = jnp.concatenate([main, tail.astype(BF)], 0)
        lhs = jnp.concatenate([table * masks[0], table * masks[1]], 0)
        rhs = jnp.concatenate([gat[kind, :, k].reshape(RR, 128), gat[kind, :, 3].reshape(RR, 128)], 1)
        sums = jnp.dot(lhs, rhs, preferred_element_type=F32)
        for h in range(2):
            first = sums[80 * h : 80 * h + 80, :128]
            second = sums[80 * h : 80 * h + 80, 128:]
            imag = jnp.where(
                lane80 < 44, pltpu.roll(first, 44, axis=1), pltpu.roll(second, (44 - 40 * k) % 128, axis=1)
            )
            for e, value in enumerate((first, imag)):
                n = 6 * h + 3 * e + k
                at = (8 * kind + n if n < 8 else 16 + 4 * kind + n - 8) * STRIDE
                fbuf[at : at + 80, :] = jnp.where(lane80 < CH, value, 0.0)

    lane24 = lax.broadcasted_iota(jnp.int32, (24, 128), 1)

    def pack(t):
        lats = []
        for i in range(LAT):
            at = 8 * t + i if i < 8 else 64 + 8 * (i - 8) + t
            lats.append(fbuf[pl.ds(at, 24, stride=STRIDE), :])
        most = jnp.abs(lats[0])
        for value in lats[1:]:
            most = jnp.maximum(most, jnp.abs(value))
        most = jnp.max(most, axis=1, keepdims=True)
        level = jnp.ceil(jnp.log2(jnp.maximum(most, 1e-30)))
        gain = jnp.exp2(15.0 - level) * SHRINK
        lats = [jnp.round(value * gain) for value in lats]
        level = jnp.broadcast_to(level, (24, 128))
        for k in range(N):
            i, skip = k + k // 4, 21 * (k % 4)
            inside = (lane24 >= skip) & (lane24 < CH)
            window = jnp.where(inside, lats[i], pltpu.roll(lats[i + 1], CH, axis=1))
            window = jnp.where(lane24 == (skip + 127) % 128, level, window).astype(jnp.int32)
            for kind in range(2):
                fsend[t, k, kind, 0:8] = window[8 * kind : 8 * kind + 8].astype(jnp.int16)
                fsend[t, k, kind, 8:12] = window[16 + 4 * kind : 20 + 4 * kind].astype(jnp.int16)

    def send_f(t):
        for n in range(0 if t else 1, N):
            m_to = (m + n) % N
            for kind in range(2):
                to = (along[kind] - t + N) % N
                pltpu.make_async_remote_copy(
                    fsend.at[t, m_to, kind], frecv.at[kind, m * N + along[kind]], fsem.at[0, kind], fsem.at[1 + kind, t],
                    device_id=device(kind, to, across[kind], m_to), device_id_type=MESH_ID,
                ).start()

    order = FAR_FIRST + (0,)
    for n, t in enumerate(order):
        pack(t)
        if n >= 1:
            send_f(order[n - 1])
    send_f(0)
    own_f = [
        pltpu.make_async_copy(fsend.at[0, m, kind], frecv.at[kind, m * N + along[kind]], own_sem.at[4 + kind])
        for kind in range(2)
    ]
    own_f[0].start()
    own_f[1].start()

    for kind in range(2):
        wait_bytes(csend.at[kind, pl.ds(0, 7)], csem.at[0, kind])
        wait_bytes(lsend.at[kind, pl.ds(0, 7)], lsem.at[0, kind])
        for way in range(2):
            for step in range(4):
                for half in range(2):
                    if step < 3 or way == half:
                        ring(kind, way, step, half).wait_send()

    turn = lax.rem(128 - 21 * lax.rem(m, 4), 128)
    for t in order:
        for kind in range(2):
            if t == 0:
                own_f[kind].wait()
            wait_bytes(frecv.at[kind, pl.ds(0, 8 if t else 7)], fsem.at[1 + kind, t])
            source = (along[kind] + t) % N
            for n in range(N):
                coded = frecv[kind, 8 * n + source].astype(jnp.int32).astype(F32)
                at = pl.multiple_of((64 * kind + 8 * n + source) * 24, 8)
                fdec[pl.ds(at, 12), :] = pltpu.roll(coded, turn, axis=1)

    lhs = []
    for h in range(2):
        at = [1536 * kind + 6 * h + 3 * e + k for e in range(2) for kind in range(2) for k in range(3)]
        rows = jnp.concatenate([fdec[pl.ds(first, 64, stride=24), :] for first in at], 0)
        rows = jnp.transpose(rows)
        rows = rows * (jnp.exp2(rows[127:128, :] - 15.0) * (1.0 / SHRINK))
        high, low = split_bf16(rows)
        lhs.append((high, jnp.concatenate([high, low], 0)))
    for l in range(3):
        at = slice(256 * l, 256 * l + 256)
        part = []
        for h in range(2):
            high, both = lhs[h]
            wide = jnp.dot(both, bas[h, 0, :, at], preferred_element_type=F32)
            part.append(
                wide[:128] + wide[128:] + jnp.dot(high, bas[h, 1, :, at], preferred_element_type=F32)
            )
        count = min(256, HALF - 256 * l)
        out[:, 256 * l : 256 * l + count] = (part[0] + part[1])[:ROWS, :count]
        out[:, HALF + 256 * l : HALF + 256 * l + count] = (part[0] - part[1])[:ROWS, :count]
    for kind in range(2):
        wait_bytes(frecv.at[kind, pl.ds(0, 63)], fsem.at[0, kind])


def body(pair_wave, legendre, coefs):
    i16 = jnp.int16
    return pl.pallas_call(
        kernel,
        out_shape=jax.ShapeDtypeStruct((ROWS, LON), F32),
        in_specs=[
            pl.BlockSpec(memory_space=pltpu.HBM),
            pl.BlockSpec(memory_space=pltpu.HBM),
            pl.BlockSpec(memory_space=pltpu.HBM),
        ],
        out_specs=pl.BlockSpec(memory_space=pltpu.VMEM),
        scratch_shapes=[
            pltpu.SMEM((360,), jnp.int32),
            pltpu.VMEM((LAT, SLOTS, RR), BF),
            pltpu.VMEM((12, SLOTS, 2 * CH), BF),
            pltpu.VMEM((RR, RR), BF),
            pltpu.VMEM((768, 128), F32),
            pltpu.VMEM((2, N, 48, 128), BF),
            pltpu.VMEM((2, N, 48, 128), BF),
            pltpu.VMEM((2, N, 4, 96, 128), BF),
            pltpu.VMEM((6, 480, 128), F32),
            pltpu.VMEM((2, N, 30, RR), BF),
            pltpu.VMEM((2, N, 30, RR), BF),
            pltpu.VMEM((2, 6, 64, 128), F32),
            pltpu.VMEM((24 * STRIDE, 128), F32),
            pltpu.VMEM((N, N, 2, 12, 128), i16),
            pltpu.VMEM((2, N * N, 12, 128), i16),
            pltpu.VMEM((2 * N * N * 24, 128), F32),
            pltpu.VMEM((384, 128), F32),
            pltpu.VMEM((2, 2, RR, RR), BF),
            pltpu.SemaphoreType.DMA((3,)),
            pltpu.SemaphoreType.DMA((6,)),
            pltpu.SemaphoreType.DMA((2, 2)),
            pltpu.SemaphoreType.DMA((2, 2)),
            pltpu.SemaphoreType.DMA((3, N)),
            pltpu.SemaphoreType.DMA((2, 2, 4, 2)),
            pltpu.SemaphoreType.DMA((2, 2, 4, 2)),
        ],
        compiler_params=pltpu.CompilerParams(collective_id=0, has_side_effects=True, vmem_limit_bytes=67043328),
    )(pair_wave, jnp.transpose(legendre, (1, 0, 2)), jnp.transpose(coefs, (1, 0, 2)))


def solution(mesh):
    split = Mesh(mesh.devices.reshape(N, N, 4, 2), ("y", "z", "x", "c"))
    placed = (P(), P(("x", "c"), ("y", "z"), None), P(("x", "c"), ("y", "z"), None))
    return jax.shard_map(
        body, mesh=split, in_specs=placed, out_specs=P(("y", "z", "x", "c"), None), check_vma=False
    )
```

```python
import math

import jax
import jax.numpy as jnp
import numpy as np
from jax import lax
from jax.experimental import pallas as pl
from jax.experimental.pallas import tpu as pltpu
from jax.sharding import Mesh
from jax.sharding import PartitionSpec as P

DEG = 720
LON = 1440
HALF = LON // 2
CH = 84
LAT = 10
SLOTS = 45
PER = 6
N = 8
ROWS = 105
PADDED = 112
RR = 768
F32 = jnp.float32
BF = jnp.bfloat16
MESH_ID = pl.DeviceIdType.MESH
FAR_FIRST = (4, 3, 5, 2, 6, 1, 7)
STRIDE = 88
BEFORE = (1, 7, 4)
BETWEEN = ((2, 6), (3, 5))
EARLY = 8
LATER = 8
SHRINK = 0.9999


def half_angle_fit():
    t = np.cos(np.linspace(0, np.pi, 4001)) * (np.pi / 2)
    sin_c = np.linalg.lstsq(np.stack([t ** (2 * i + 1) for i in range(5)], 1), np.sin(t), rcond=None)[0]
    cos_c = np.linalg.lstsq(np.stack([t ** (2 * i) for i in range(6)], 1), np.cos(t), rcond=None)[0]
    return [float(v) for v in sin_c], [float(v) for v in cos_c]


SIN_C, COS_C = half_angle_fit()


def horner(coefs, square):
    total = jnp.full_like(square, coefs[-1])
    for value in coefs[-2::-1]:
        total = total * square + value
    return total


def wave_rows(waves, weight, lon_at):
    product = waves * lon_at
    turns = jnp.round(product * (1.0 / LON))
    half = (product - turns * float(LON)) * (math.pi / LON)
    square = half * half
    sine = half * horner(SIN_C, square)
    cosine = horner(COS_C, square)
    twice = (2.0 * weight) * sine
    return weight - twice * sine, -twice * cosine


def split_bf16(x):
    high = x.astype(BF)
    return high, (x - high.astype(F32)).astype(BF)


def natural_rows():
    lane = lax.broadcasted_iota(jnp.int32, (1, RR), 1).astype(F32)
    z_at = jnp.floor((lane + 0.5) * (1.0 / 96))
    rest = lane - 96.0 * z_at
    y_at = jnp.floor((rest + 0.5) * (1.0 / 12))
    return lane, (8.0 * y_at + z_at) * 12.0 + rest - 12.0 * y_at


def kernel(
    pw_hbm, leg_hbm, cf_hbm, out,
    pw, leg, cf, perm, cbuf, csend, crecv, gat, lbuf, lsend, lrecv, ltail, fbuf, fsend, frecv, fdec, ucol, bas,
    in_sem, own_sem, csem, lsem, fsem, ring_s, ring_r,
):
    y, z = lax.axis_index("y"), lax.axis_index("z")
    m = 2 * lax.axis_index("x") + lax.axis_index("c")
    along, across = (z, y), (y, z)

    def device(kind, along_at, across_at, m_at):
        place = (across_at, along_at) if kind == 0 else (along_at, across_at)
        return (*place, m_at // 2, m_at % 2)

    barrier = pltpu.get_barrier_semaphore()
    peers = [device(kind, (along[kind] + t) % N, across[kind], m) for t in FAR_FIRST for kind in range(2)]
    peers += [device(0, z, y, (m + t) % N) for t in FAR_FIRST]
    for peer in peers:
        pl.semaphore_signal(barrier, inc=1, device_id=peer, device_id_type=MESH_ID)
    cf_in = pltpu.make_async_copy(cf_hbm, cf, in_sem.at[0])
    leg_in = pltpu.make_async_copy(leg_hbm, leg, in_sem.at[1])
    pw_in = pltpu.make_async_copy(pw_hbm, pw, in_sem.at[2])
    cf_in.start()
    leg_in.start()
    pw_in.start()

    lane_row, natural = natural_rows()

    @pl.loop(0, 48)
    def _(block):
        row = lax.broadcasted_iota(jnp.int32, (16, RR), 0).astype(F32) + (16 * block).astype(F32)
        perm[pl.ds(pl.multiple_of(block * 16, 16), 16), :] = jnp.where(row == natural, 1.0, 0.0).astype(BF)

    def slot_tile(ref, row, j):
        count = min(8, SLOTS - 8 * j)
        tile = ref[row, 8 * j : 8 * j + count, :].astype(F32)
        if count < 8:
            tile = jnp.concatenate([tile, jnp.zeros((8 - count, tile.shape[1]), F32)], 0)
        return tile

    cf_in.wait()
    for r in range(12):
        for g in range(2):
            tiles = [slot_tile(cf, r, 3 * g + k) for k in range(3)]
            at = 8 * (48 * g + 4 * r)
            for k in range(3):
                cbuf[at + 8 * k : at + 8 * k + 8, :] = tiles[k][:, :128]
            rest = [t[:, 128:] for t in tiles] + [jnp.zeros((8, 8), F32)]
            cbuf[at + 24 : at + 32, :] = jnp.concatenate(rest, 1)
    for g in range(2):
        for d in range(N):
            csend[g, d] = cbuf[pl.ds(384 * g + d, 48, stride=8), :].astype(BF)

    def put_leg(kind, i, k, tile):
        at = 240 * kind + 8 * (8 * k + i if i < 8 else 24 + 2 * k + i - 8)
        for l in range(6):
            lbuf[l, at : at + 8, :] = tile[:, 128 * l : 128 * l + 128]

    def pack_leg(kind):
        for d in range(N):
            for l in range(6):
                rows = lbuf[l, pl.ds(240 * kind + d, 30, stride=8), :]
                lsend[kind, d, :, 128 * l : 128 * l + 128] = rows.astype(BF)

    leg_in.wait()
    for i in range(LAT):
        for k in range(3):
            put_leg(0, i, k, slot_tile(leg, i, k))
    pack_leg(0)

    pl.semaphore_wait(barrier, len(peers))

    own_c = pltpu.make_async_copy(
        csend.at[0, along[0]], crecv.at[0, along[0]], own_sem.at[0]
    ), pltpu.make_async_copy(csend.at[1, along[1]], crecv.at[1, along[1]], own_sem.at[1])
    for t in FAR_FIRST:
        for kind in range(2):
            to = (along[kind] + t) % N
            pltpu.make_async_remote_copy(
                csend.at[kind, to], crecv.at[kind, along[kind]], csem.at[0, kind], csem.at[1, kind],
                device_id=device(kind, to, across[kind], m), device_id_type=MESH_ID,
            ).start()
    own_c[0].start()
    own_c[1].start()

    def send_leg(t):
        for kind in range(2):
            to = (along[kind] + t) % N
            pltpu.make_async_remote_copy(
                lsend.at[kind, to], lrecv.at[kind, t], lsem.at[0, kind], lsem.at[1, kind],
                device_id=device(kind, to, across[kind], m), device_id_type=MESH_ID,
            ).start()

    rows = [jnp.concatenate([slot_tile(leg, i, 3 + k) for k in range(3)], 0).astype(BF) for i in range(LAT)]
    moved = jnp.dot(jnp.concatenate(rows, 0), perm[...], preferred_element_type=F32)
    for i in range(LAT):
        for k in range(3):
            put_leg(1, i, k, moved[24 * i + 8 * k : 24 * i + 8 * k + 8])
    pack_leg(1)
    for t in BEFORE:
        send_leg(t)
    pw_in.wait()

    @pl.loop(0, PER * N)
    def _(tile):
        first = SLOTS * (tile % N) + 8 * (tile // N)
        rows = [jnp.full((1, 128), pw[jnp.minimum(first + d, 359)].astype(F32)) for d in range(8)]
        ucol[pl.ds(pl.multiple_of(tile * 8, 8), 8), :] = jnp.concatenate(rows, 0)

    lane = lax.broadcasted_iota(jnp.int32, (16, 128), 1).astype(F32)

    def make_basis(first, last):
        @pl.loop(first, last)
        def _(block):
            at = pl.multiple_of(block * 16, 16)
            u = ucol[pl.ds(at, 16), :]
            odd = u - 2.0 * jnp.floor(u * 0.5) > 0.5
            even_wave = jnp.where(odd, float(DEG - 1) - u, u)
            weight = jnp.where(even_wave == 0.0, 1.0, 2.0)
            for h, (wave, wt) in enumerate(((even_wave, weight), (float(DEG - 1) - even_wave, 2.0))):
                for l in range(6):
                    pair = wave_rows(wave, wt, lane + 128.0 * l)
                    for e in range(2):
                        high, low = split_bf16(pair[e])
                        to = pl.multiple_of(384 * e + at, 16)
                        bas[h, 0, pl.ds(to, 16), 128 * l : 128 * l + 128] = high
                        bas[h, 1, pl.ds(to, 16), 128 * l : 128 * l + 128] = low

    own_l = [
        pltpu.make_async_copy(lsend.at[kind, along[kind]], lrecv.at[kind, 0], own_sem.at[2 + kind])
        for kind in range(2)
    ]
    own_l[0].start()
    own_l[1].start()
    make_basis(0, EARLY)

    def wait_bytes(ref, sem):
        pltpu.make_async_copy(ref, ref, sem).wait()

    def ring(kind, way, step, half):
        own, back, on = across[kind], min(step, 2), 1 + step // 3
        origin = (own - back + N) % N if way == 0 else (own + back) % N
        part = gat.at[kind, origin, pl.ds(2 * half, 2)]
        to = (own + on) % N if way == 0 else (own + N - on) % N
        return pltpu.make_async_remote_copy(
            part, part, ring_s.at[kind, way, step, half], ring_r.at[kind, way, step, half],
            device_id=device(kind, along[kind], to, m), device_id_type=MESH_ID,
        )

    for kind in range(2):
        own_c[kind].wait()
        wait_bytes(crecv.at[kind, pl.ds(0, 7)], csem.at[1, kind])
        for s in range(N):
            cbuf[48 * s : 48 * s + 48, :] = crecv[kind, s].astype(F32)
        for blk in range(4):
            gat[kind, across[kind], blk] = cbuf[pl.ds(blk, 96, stride=4), :].astype(BF)
        for half in range(2):
            for way in range(2):
                ring(kind, way, 0, half).start()
    for step in range(1, 3):
        for t in BETWEEN[step - 1]:
            send_leg(t)
        make_basis(EARLY + LATER * (step - 1), min(24, EARLY + LATER * step))
        for half in range(2):
            for kind in range(2):
                for way in range(2):
                    ring(kind, way, step - 1, half).wait_recv()
                    if step == 2 and way == half:
                        ring(kind, way, 3, half).start()
                    ring(kind, way, step, half).start()
    for kind in range(2):
        own_l[kind].wait()
        wait_bytes(lrecv.at[kind, pl.ds(0, 7)], lsem.at[1, kind])
        for t in range(N):
            for l in range(6):
                ltail[kind, l, 8 * t : 8 * t + 6, :] = lrecv[kind, t, 24:30, 128 * l : 128 * l + 128].astype(F32)
    for kind in range(2):
        for way in range(2):
            for half in range(2):
                ring(kind, way, 2, half).wait_recv()
            ring(kind, way, 3, way).wait_recv()

    lane80 = lax.broadcasted_iota(jnp.int32, (80, 128), 1)
    for j in range(PER):
        kind, k = divmod(j, 3)
        u = pw[SLOTS * m + jnp.minimum(8 * j + along[kind], SLOTS - 1)]
        row_at = natural if kind else lane_row
        low = (row_at < (DEG - u).astype(F32)).astype(F32)
        high = (row_at <= float(DEG)).astype(F32) - low
        swap = lax.rem(u, 2).astype(F32)
        masks = [(low + swap * (high - low)).astype(BF), (high + swap * (low - high)).astype(BF)]
        main = lrecv[kind, :, 8 * k : 8 * k + 8, :].reshape(64, RR)
        tail = [[ltail[kind, l, pl.ds(2 * k + n, 8, stride=8), :] for l in range(6)] for n in range(2)]
        tail = jnp.concatenate([jnp.concatenate(t, 1) for t in tail], 0)
        table = jnp.concatenate([main, tail.astype(BF)], 0)
        lhs = jnp.concatenate([table * masks[0], table * masks[1]], 0)
        rhs = jnp.concatenate([gat[kind, :, k].reshape(RR, 128), gat[kind, :, 3].reshape(RR, 128)], 1)
        sums = jnp.dot(lhs, rhs, preferred_element_type=F32)
        for h in range(2):
            first = sums[80 * h : 80 * h + 80, :128]
            second = sums[80 * h : 80 * h + 80, 128:]
            imag = jnp.where(
                lane80 < 44, pltpu.roll(first, 44, axis=1), pltpu.roll(second, (44 - 40 * k) % 128, axis=1)
            )
            for e, value in enumerate((first, imag)):
                n = 6 * h + 3 * e + k
                at = (8 * kind + n if n < 8 else 16 + 4 * kind + n - 8) * STRIDE
                fbuf[at : at + 80, :] = jnp.where(lane80 < CH, value, 0.0)

    lane24 = lax.broadcasted_iota(jnp.int32, (24, 128), 1)

    def lats_of(t):
        at = [8 * t + i if i < 8 else 64 + 8 * (i - 8) + t for i in range(LAT)]
        return [fbuf[pl.ds(first, 24, stride=STRIDE), :] for first in at]

    def level_of(t):
        most = [jnp.abs(value) for value in lats_of(t)]
        while len(most) > 1:
            most = [jnp.maximum(a, b) for a, b in zip(most[::2], most[1::2])] + most[len(most) // 2 * 2 :]
        return jnp.ceil(jnp.log2(jnp.maximum(jnp.max(most[0], axis=1, keepdims=True), 1e-30)))

    def pack(t):
        gain = jnp.exp2(15.0 - levels[t]) * SHRINK
        lats = [jnp.round(value * gain) for value in lats_of(t)]
        level = jnp.broadcast_to(levels[t], (24, 128))
        for k in range(N):
            i, skip = k + k // 4, 21 * (k % 4)
            inside = (lane24 >= skip) & (lane24 < CH)
            window = jnp.where(inside, lats[i], pltpu.roll(lats[i + 1], CH, axis=1))
            window = jnp.where(lane24 == (skip + 127) % 128, level, window).astype(jnp.int32)
            for kind in range(2):
                fsend[t, k, kind, 0:8] = window[8 * kind : 8 * kind + 8].astype(jnp.int16)
                fsend[t, k, kind, 8:12] = window[16 + 4 * kind : 20 + 4 * kind].astype(jnp.int16)

    def send_f(t):
        for n in range(0 if t else 1, N):
            m_to = (m + n) % N
            for kind in range(2):
                to = (along[kind] - t + N) % N
                pltpu.make_async_remote_copy(
                    fsend.at[t, m_to, kind], frecv.at[kind, m * N + along[kind]], fsem.at[0, kind], fsem.at[1 + kind, t],
                    device_id=device(kind, to, across[kind], m_to), device_id_type=MESH_ID,
                ).start()

    order = FAR_FIRST + (0,)
    levels = {t: level_of(t) for t in order}
    for n, t in enumerate(order):
        pack(t)
        if n >= 1:
            send_f(order[n - 1])
    send_f(0)
    own_f = [
        pltpu.make_async_copy(fsend.at[0, m, kind], frecv.at[kind, m * N + along[kind]], own_sem.at[4 + kind])
        for kind in range(2)
    ]
    own_f[0].start()
    own_f[1].start()

    for kind in range(2):
        wait_bytes(csend.at[kind, pl.ds(0, 7)], csem.at[0, kind])
        wait_bytes(lsend.at[kind, pl.ds(0, 7)], lsem.at[0, kind])
        for way in range(2):
            for step in range(4):
                for half in range(2):
                    if step < 3 or way == half:
                        ring(kind, way, step, half).wait_send()

    turn = lax.rem(128 - 21 * lax.rem(m, 4), 128)
    for t in order:
        for kind in range(2):
            if t == 0:
                own_f[kind].wait()
            wait_bytes(frecv.at[kind, pl.ds(0, 8 if t else 7)], fsem.at[1 + kind, t])
            source = (along[kind] + t) % N
            for n in range(N):
                coded = frecv[kind, 8 * n + source].astype(jnp.int32).astype(F32)
                at = pl.multiple_of((64 * kind + 8 * n + source) * 24, 8)
                fdec[pl.ds(at, 12), :] = pltpu.roll(coded, turn, axis=1)

    lhs = []
    for h in range(2):
        at = [1536 * kind + 6 * h + 3 * e + k for e in range(2) for kind in range(2) for k in range(3)]
        rows = jnp.concatenate([fdec[pl.ds(first, 64, stride=24), :] for first in at], 0)
        rows = jnp.transpose(rows)
        rows = rows[:PADDED] * (jnp.exp2(rows[127:128, :] - 15.0) * (1.0 / SHRINK))
        high, low = split_bf16(rows)
        lhs.append((high, jnp.concatenate([high, low], 0)))
    for l in range(3):
        at = slice(256 * l, 256 * l + 256)
        part = []
        for h in range(2):
            high, both = lhs[h]
            wide = jnp.dot(both, bas[h, 0, :, at], preferred_element_type=F32)
            part.append(
                wide[:PADDED] + wide[PADDED:] + jnp.dot(high, bas[h, 1, :, at], preferred_element_type=F32)
            )
        count = min(256, HALF - 256 * l)
        out[:, 256 * l : 256 * l + count] = (part[0] + part[1])[:ROWS, :count]
        out[:, HALF + 256 * l : HALF + 256 * l + count] = (part[0] - part[1])[:ROWS, :count]
    for kind in range(2):
        wait_bytes(frecv.at[kind, pl.ds(0, 63)], fsem.at[0, kind])


def body(pair_wave, legendre, coefs):
    i16 = jnp.int16
    return pl.pallas_call(
        kernel,
        out_shape=pltpu.VMEM((ROWS, LON), F32),
        in_specs=[
            pl.BlockSpec(memory_space=pltpu.HBM),
            pl.BlockSpec(memory_space=pltpu.HBM),
            pl.BlockSpec(memory_space=pltpu.HBM),
        ],
        out_specs=pl.BlockSpec(memory_space=pltpu.VMEM),
        scratch_shapes=[
            pltpu.SMEM((360,), jnp.int32),
            pltpu.VMEM((LAT, SLOTS, RR), BF),
            pltpu.VMEM((12, SLOTS, 2 * CH), BF),
            pltpu.VMEM((RR, RR), BF),
            pltpu.VMEM((768, 128), F32),
            pltpu.VMEM((2, N, 48, 128), BF),
            pltpu.VMEM((2, N, 48, 128), BF),
            pltpu.VMEM((2, N, 4, 96, 128), BF),
            pltpu.VMEM((6, 480, 128), F32),
            pltpu.VMEM((2, N, 30, RR), BF),
            pltpu.VMEM((2, N, 30, RR), BF),
            pltpu.VMEM((2, 6, 64, 128), F32),
            pltpu.VMEM((24 * STRIDE, 128), F32),
            pltpu.VMEM((N, N, 2, 12, 128), i16),
            pltpu.VMEM((2, N * N, 12, 128), i16),
            pltpu.VMEM((2 * N * N * 24, 128), F32),
            pltpu.VMEM((384, 128), F32),
            pltpu.VMEM((2, 2, RR, RR), BF),
            pltpu.SemaphoreType.DMA((3,)),
            pltpu.SemaphoreType.DMA((6,)),
            pltpu.SemaphoreType.DMA((2, 2)),
            pltpu.SemaphoreType.DMA((2, 2)),
            pltpu.SemaphoreType.DMA((3, N)),
            pltpu.SemaphoreType.DMA((2, 2, 4, 2)),
            pltpu.SemaphoreType.DMA((2, 2, 4, 2)),
        ],
        compiler_params=pltpu.CompilerParams(collective_id=0, has_side_effects=True, vmem_limit_bytes=62000000),
    )(pair_wave, jnp.transpose(legendre, (1, 0, 2)), jnp.transpose(coefs, (1, 0, 2)))


def solution(mesh):
    split = Mesh(mesh.devices.reshape(N, N, 4, 2), ("y", "z", "x", "c"))
    placed = (P(), P(("x", "c"), ("y", "z"), None), P(("x", "c"), ("y", "z"), None))
    return jax.shard_map(
        body, mesh=split, in_specs=placed, out_specs=P(("y", "z", "x", "c"), None), check_vma=False
    )
```

```python
import math

import jax
import jax.numpy as jnp
import numpy as np
from jax import lax
from jax.experimental import pallas as pl
from jax.experimental.pallas import tpu as pltpu
from jax.sharding import Mesh
from jax.sharding import PartitionSpec as P

DEG = 720
LON = 1440
HALF = LON // 2
CH = 84
LAT = 10
SLOTS = 45
PER = 6
N = 8
ROWS = 105
PADDED = 112
RR = 768
F32 = jnp.float32
BF = jnp.bfloat16
MESH_ID = pl.DeviceIdType.MESH
FAR_FIRST = (4, 3, 5, 2, 6, 1, 7)
STRIDE = 88
BEFORE = (1, 7, 4)
BETWEEN = ((2, 6), (3, 5))
EARLY = 8
LATER = 8
SHRINK = 0.9999


def half_angle_fit():
    t = np.cos(np.linspace(0, np.pi, 4001)) * (np.pi / 2)
    sin_c = np.linalg.lstsq(np.stack([t ** (2 * i + 1) for i in range(5)], 1), np.sin(t), rcond=None)[0]
    cos_c = np.linalg.lstsq(np.stack([t ** (2 * i) for i in range(6)], 1), np.cos(t), rcond=None)[0]
    return [float(v) for v in sin_c], [float(v) for v in cos_c]


SIN_C, COS_C = half_angle_fit()


def horner(coefs, square):
    total = jnp.full_like(square, coefs[-1])
    for value in coefs[-2::-1]:
        total = total * square + value
    return total


def wave_rows(waves, weight, lon_at):
    product = waves * lon_at
    turns = jnp.round(product * (1.0 / LON))
    half = (product - turns * float(LON)) * (math.pi / LON)
    square = half * half
    sine = half * horner(SIN_C, square)
    cosine = horner(COS_C, square)
    twice = (2.0 * weight) * sine
    return weight - twice * sine, -twice * cosine


def split_bf16(x):
    high = x.astype(BF)
    return high, (x - high.astype(F32)).astype(BF)


def natural_rows():
    lane = lax.broadcasted_iota(jnp.int32, (1, RR), 1).astype(F32)
    z_at = jnp.floor((lane + 0.5) * (1.0 / 96))
    rest = lane - 96.0 * z_at
    y_at = jnp.floor((rest + 0.5) * (1.0 / 12))
    return lane, (8.0 * y_at + z_at) * 12.0 + rest - 12.0 * y_at


def kernel(
    pw_hbm, leg_hbm, cf_hbm, out,
    pw, leg, cf, perm, cbuf, csend, crecv, gat, lbuf, lsend, lrecv, ltail, fbuf, fsend, frecv, fdec, ucol, bas,
    in_sem, own_sem, csem, lsem, fsem, ring_s, ring_r,
):
    y, z = lax.axis_index("y"), lax.axis_index("z")
    m = 2 * lax.axis_index("x") + lax.axis_index("c")
    along, across = (z, y), (y, z)

    def device(kind, along_at, across_at, m_at):
        place = (across_at, along_at) if kind == 0 else (along_at, across_at)
        return (*place, m_at // 2, m_at % 2)

    barrier = pltpu.get_barrier_semaphore()
    peers = [device(kind, (along[kind] + t) % N, across[kind], m) for t in FAR_FIRST for kind in range(2)]
    peers += [device(0, z, y, (m + t) % N) for t in FAR_FIRST]
    for peer in peers:
        pl.semaphore_signal(barrier, inc=1, device_id=peer, device_id_type=MESH_ID)
    cf_in = pltpu.make_async_copy(cf_hbm, cf, in_sem.at[0])
    leg_in = pltpu.make_async_copy(leg_hbm, leg, in_sem.at[1])
    pw_in = pltpu.make_async_copy(pw_hbm, pw, in_sem.at[2])
    cf_in.start()
    leg_in.start()
    pw_in.start()

    lane_row, natural = natural_rows()

    @pl.loop(0, 48)
    def _(block):
        row = lax.broadcasted_iota(jnp.int32, (16, RR), 0).astype(F32) + (16 * block).astype(F32)
        perm[pl.ds(pl.multiple_of(block * 16, 16), 16), :] = jnp.where(row == natural, 1.0, 0.0).astype(BF)

    def slot_tile(ref, row, j):
        count = min(8, SLOTS - 8 * j)
        tile = ref[row, 8 * j : 8 * j + count, :].astype(F32)
        if count < 8:
            tile = jnp.concatenate([tile, jnp.zeros((8 - count, tile.shape[1]), F32)], 0)
        return tile

    cf_in.wait()
    for r in range(12):
        for g in range(2):
            tiles = [slot_tile(cf, r, 3 * g + k) for k in range(3)]
            at = 8 * (48 * g + 4 * r)
            for k in range(3):
                cbuf[at + 8 * k : at + 8 * k + 8, :] = tiles[k][:, :128]
            rest = [t[:, 128:] for t in tiles] + [jnp.zeros((8, 8), F32)]
            cbuf[at + 24 : at + 32, :] = jnp.concatenate(rest, 1)
    for g in range(2):
        for d in range(N):
            csend[g, d] = cbuf[pl.ds(384 * g + d, 48, stride=8), :].astype(BF)

    def put_leg(kind, i, k, tile):
        at = 240 * kind + 8 * (8 * k + i if i < 8 else 24 + 2 * k + i - 8)
        for l in range(6):
            lbuf[l, at : at + 8, :] = tile[:, 128 * l : 128 * l + 128]

    def pack_leg(kind):
        for d in range(N):
            for l in range(6):
                rows = lbuf[l, pl.ds(240 * kind + d, 30, stride=8), :]
                lsend[kind, d, :, 128 * l : 128 * l + 128] = rows.astype(BF)

    leg_in.wait()
    for i in range(LAT):
        for k in range(3):
            put_leg(0, i, k, slot_tile(leg, i, k))
    pack_leg(0)

    pl.semaphore_wait(barrier, len(peers))

    own_c = pltpu.make_async_copy(
        csend.at[0, along[0]], crecv.at[0, along[0]], own_sem.at[0]
    ), pltpu.make_async_copy(csend.at[1, along[1]], crecv.at[1, along[1]], own_sem.at[1])
    for t in FAR_FIRST:
        for kind in range(2):
            to = (along[kind] + t) % N
            pltpu.make_async_remote_copy(
                csend.at[kind, to], crecv.at[kind, along[kind]], csem.at[0, kind], csem.at[1, kind],
                device_id=device(kind, to, across[kind], m), device_id_type=MESH_ID,
            ).start()
    own_c[0].start()
    own_c[1].start()

    def send_leg(t):
        for kind in range(2):
            to = (along[kind] + t) % N
            pltpu.make_async_remote_copy(
                lsend.at[kind, to], lrecv.at[kind, t], lsem.at[0, kind], lsem.at[1, kind],
                device_id=device(kind, to, across[kind], m), device_id_type=MESH_ID,
            ).start()

    rows = [jnp.concatenate([slot_tile(leg, i, 3 + k) for k in range(3)], 0).astype(BF) for i in range(LAT)]
    moved = jnp.dot(jnp.concatenate(rows, 0), perm[...], preferred_element_type=F32)
    for i in range(LAT):
        for k in range(3):
            put_leg(1, i, k, moved[24 * i + 8 * k : 24 * i + 8 * k + 8])
    pack_leg(1)
    for t in BEFORE:
        send_leg(t)
    pw_in.wait()

    @pl.loop(0, PER * N)
    def _(tile):
        first = SLOTS * (tile % N) + 8 * (tile // N)
        rows = [jnp.full((1, 128), pw[jnp.minimum(first + d, 359)].astype(F32)) for d in range(8)]
        ucol[pl.ds(pl.multiple_of(tile * 8, 8), 8), :] = jnp.concatenate(rows, 0)

    lane = lax.broadcasted_iota(jnp.int32, (16, 128), 1).astype(F32)

    def make_basis(first, last):
        @pl.loop(first, last)
        def _(block):
            at = pl.multiple_of(block * 16, 16)
            u = ucol[pl.ds(at, 16), :]
            odd = u - 2.0 * jnp.floor(u * 0.5) > 0.5
            even_wave = jnp.where(odd, float(DEG - 1) - u, u)
            weight = jnp.where(even_wave == 0.0, 1.0, 2.0)
            for h, (wave, wt) in enumerate(((even_wave, weight), (float(DEG - 1) - even_wave, 2.0))):
                for l in range(6):
                    pair = wave_rows(wave, wt, lane + 128.0 * l)
                    for e in range(2):
                        high, low = split_bf16(pair[e])
                        to = pl.multiple_of(384 * e + at, 16)
                        bas[h, 0, pl.ds(to, 16), 128 * l : 128 * l + 128] = high
                        bas[h, 1, pl.ds(to, 16), 128 * l : 128 * l + 128] = low

    own_l = [
        pltpu.make_async_copy(lsend.at[kind, along[kind]], lrecv.at[kind, 0], own_sem.at[2 + kind])
        for kind in range(2)
    ]
    own_l[0].start()
    own_l[1].start()
    make_basis(0, EARLY)

    def wait_bytes(ref, sem):
        pltpu.make_async_copy(ref, ref, sem).wait()

    def ring(kind, way, step, half):
        own, back, on = across[kind], min(step, 2), 1 + step // 3
        origin = (own - back + N) % N if way == 0 else (own + back) % N
        part = gat.at[kind, origin, pl.ds(2 * half, 2)]
        to = (own + on) % N if way == 0 else (own + N - on) % N
        return pltpu.make_async_remote_copy(
            part, part, ring_s.at[kind, way, step, half], ring_r.at[kind, way, step, half],
            device_id=device(kind, along[kind], to, m), device_id_type=MESH_ID,
        )

    for kind in range(2):
        own_c[kind].wait()
        wait_bytes(crecv.at[kind, pl.ds(0, 7)], csem.at[1, kind])
        for s in range(N):
            cbuf[48 * s : 48 * s + 48, :] = crecv[kind, s].astype(F32)
        for blk in range(4):
            gat[kind, across[kind], blk] = cbuf[pl.ds(blk, 96, stride=4), :].astype(BF)
        for half in range(2):
            for way in range(2):
                ring(kind, way, 0, half).start()
    for step in range(1, 3):
        for t in BETWEEN[step - 1]:
            send_leg(t)
        make_basis(EARLY + LATER * (step - 1), min(24, EARLY + LATER * step))
        for half in range(2):
            for kind in range(2):
                for way in range(2):
                    ring(kind, way, step - 1, half).wait_recv()
                    if step == 2 and way == half:
                        ring(kind, way, 3, half).start()
                    ring(kind, way, step, half).start()
    for kind in range(2):
        own_l[kind].wait()
        wait_bytes(lrecv.at[kind, pl.ds(0, 7)], lsem.at[1, kind])
        for t in range(N):
            for l in range(6):
                ltail[kind, l, 8 * t : 8 * t + 6, :] = lrecv[kind, t, 24:30, 128 * l : 128 * l + 128].astype(F32)
    for kind in range(2):
        for way in range(2):
            for half in range(2):
                ring(kind, way, 2, half).wait_recv()
            ring(kind, way, 3, way).wait_recv()

    lane80 = lax.broadcasted_iota(jnp.int32, (80, 128), 1)
    for j in range(PER):
        kind, k = divmod(j, 3)
        u = pw[SLOTS * m + jnp.minimum(8 * j + along[kind], SLOTS - 1)]
        row_at = natural if kind else lane_row
        low = (row_at < (DEG - u).astype(F32)).astype(F32)
        high = (row_at <= float(DEG)).astype(F32) - low
        swap = lax.rem(u, 2).astype(F32)
        masks = [(low + swap * (high - low)).astype(BF), (high + swap * (low - high)).astype(BF)]
        main = lrecv[kind, :, 8 * k : 8 * k + 8, :].reshape(64, RR)
        tail = [[ltail[kind, l, pl.ds(2 * k + n, 8, stride=8), :] for l in range(6)] for n in range(2)]
        tail = jnp.concatenate([jnp.concatenate(t, 1) for t in tail], 0)
        table = jnp.concatenate([main, tail.astype(BF)], 0)
        lhs = jnp.concatenate([table * masks[0], table * masks[1]], 0)
        rhs = jnp.concatenate([gat[kind, :, k].reshape(RR, 128), gat[kind, :, 3].reshape(RR, 128)], 1)
        sums = jnp.dot(lhs, rhs, preferred_element_type=F32)
        for h in range(2):
            first = sums[80 * h : 80 * h + 80, :128]
            second = sums[80 * h : 80 * h + 80, 128:]
            imag = jnp.where(
                lane80 < 44, pltpu.roll(first, 44, axis=1), pltpu.roll(second, (44 - 40 * k) % 128, axis=1)
            )
            for e, value in enumerate((first, imag)):
                at = (16 * kind + 8 * h + 3 * e + k) * STRIDE
                fbuf[at : at + 80, :] = jnp.where(lane80 < CH, value, 0.0)

    lane8 = lax.broadcasted_iota(jnp.int32, (8, 128), 1)

    def lats_of(t):
        at = [8 * t + i if i < 8 else 64 + 8 * (i - 8) + t for i in range(LAT)]
        return [fbuf[pl.ds(first, 32, stride=STRIDE), :] for first in at]

    def level_of(t):
        most = [jnp.abs(value) for value in lats_of(t)]
        while len(most) > 1:
            most = [jnp.maximum(a, b) for a, b in zip(most[::2], most[1::2])] + most[len(most) // 2 * 2 :]
        return jnp.ceil(jnp.log2(jnp.maximum(jnp.max(most[0], axis=1, keepdims=True), 1e-30)))

    def words(value):
        whole = value.astype(jnp.int32)
        return [(whole[at : at + 8] & 0xFFFF) | (whole[at + 8 : at + 16] << 16) for at in (0, 16)]

    def pack(t):
        gain = jnp.exp2(15.0 - levels[t]) * SHRINK
        lats = [words(jnp.round(value * gain)) for value in lats_of(t)]
        level = words(jnp.broadcast_to(levels[t], (32, 128)))
        for k in range(N):
            i, skip = k + k // 4, 21 * (k % 4)
            inside = (lane8 >= skip) & (lane8 < CH)
            for kind in range(2):
                window = jnp.where(inside, lats[i][kind], pltpu.roll(lats[i + 1][kind], CH, axis=1))
                window = jnp.where(lane8 == (skip + 127) % 128, level[kind], window)
                fsend[t, k, kind] = window[:PER]

    def send_f(t):
        for n in range(0 if t else 1, N):
            m_to = (m + n) % N
            for kind in range(2):
                to = (along[kind] - t + N) % N
                pltpu.make_async_remote_copy(
                    fsend.at[t, m_to, kind], frecv.at[kind, m * N + along[kind]], fsem.at[0, kind], fsem.at[1 + kind, t],
                    device_id=device(kind, to, across[kind], m_to), device_id_type=MESH_ID,
                ).start()

    order = FAR_FIRST + (0,)
    levels = {t: level_of(t) for t in order}
    for n, t in enumerate(order):
        pack(t)
        if n >= 1:
            send_f(order[n - 1])
    send_f(0)
    own_f = [
        pltpu.make_async_copy(fsend.at[0, m, kind], frecv.at[kind, m * N + along[kind]], own_sem.at[4 + kind])
        for kind in range(2)
    ]
    own_f[0].start()
    own_f[1].start()

    for kind in range(2):
        wait_bytes(csend.at[kind, pl.ds(0, 7)], csem.at[0, kind])
        wait_bytes(lsend.at[kind, pl.ds(0, 7)], lsem.at[0, kind])
        for way in range(2):
            for step in range(4):
                for half in range(2):
                    if step < 3 or way == half:
                        ring(kind, way, step, half).wait_send()

    turn = lax.rem(128 - 21 * lax.rem(m, 4), 128)
    for t in order:
        for kind in range(2):
            if t == 0:
                own_f[kind].wait()
            wait_bytes(frecv.at[kind, pl.ds(0, 8 if t else 7)], fsem.at[1 + kind, t])
            source = (along[kind] + t) % N
            for n in range(N):
                coded = pltpu.roll(frecv[kind, 8 * n + source], turn, axis=1)
                at = pl.multiple_of((64 * kind + 8 * n + source) * 8, 8)
                fdec[pl.ds(at, PER), :] = ((coded << 16) >> 16).astype(F32)
                fdec[pl.ds(1024 + at, PER), :] = (coded >> 16).astype(F32)

    lhs = []
    for h in range(2):
        at = [1024 * h + 512 * kind + 3 * e + k for e in range(2) for kind in range(2) for k in range(3)]
        rows = jnp.concatenate([fdec[pl.ds(first, 64, stride=8), :] for first in at], 0)
        rows = jnp.transpose(rows)
        rows = rows[:PADDED] * (jnp.exp2(rows[127:128, :] - 15.0) * (1.0 / SHRINK))
        high, low = split_bf16(rows)
        lhs.append((high, jnp.concatenate([high, low], 0)))
    for l in range(3):
        at = slice(256 * l, 256 * l + 256)
        part = []
        for h in range(2):
            high, both = lhs[h]
            wide = jnp.dot(both, bas[h, 0, :, at], preferred_element_type=F32)
            part.append(
                wide[:PADDED] + wide[PADDED:] + jnp.dot(high, bas[h, 1, :, at], preferred_element_type=F32)
            )
        count = min(256, HALF - 256 * l)
        out[:, 256 * l : 256 * l + count] = (part[0] + part[1])[:ROWS, :count]
        out[:, HALF + 256 * l : HALF + 256 * l + count] = (part[0] - part[1])[:ROWS, :count]
    for kind in range(2):
        wait_bytes(frecv.at[kind, pl.ds(0, 63)], fsem.at[0, kind])


def body(pair_wave, legendre, coefs):
    return pl.pallas_call(
        kernel,
        out_shape=pltpu.VMEM((ROWS, LON), F32),
        in_specs=[
            pl.BlockSpec(memory_space=pltpu.HBM),
            pl.BlockSpec(memory_space=pltpu.HBM),
            pl.BlockSpec(memory_space=pltpu.HBM),
        ],
        out_specs=pl.BlockSpec(memory_space=pltpu.VMEM),
        scratch_shapes=[
            pltpu.SMEM((360,), jnp.int32),
            pltpu.VMEM((LAT, SLOTS, RR), BF),
            pltpu.VMEM((12, SLOTS, 2 * CH), BF),
            pltpu.VMEM((RR, RR), BF),
            pltpu.VMEM((768, 128), F32),
            pltpu.VMEM((2, N, 48, 128), BF),
            pltpu.VMEM((2, N, 48, 128), BF),
            pltpu.VMEM((2, N, 4, 96, 128), BF),
            pltpu.VMEM((6, 480, 128), F32),
            pltpu.VMEM((2, N, 30, RR), BF),
            pltpu.VMEM((2, N, 30, RR), BF),
            pltpu.VMEM((2, 6, 64, 128), F32),
            pltpu.VMEM((32 * STRIDE, 128), F32),
            pltpu.VMEM((N, N, 2, PER, 128), jnp.int32),
            pltpu.VMEM((2, N * N, PER, 128), jnp.int32),
            pltpu.VMEM((2 * 2 * N * N * 8, 128), F32),
            pltpu.VMEM((384, 128), F32),
            pltpu.VMEM((2, 2, RR, RR), BF),
            pltpu.SemaphoreType.DMA((3,)),
            pltpu.SemaphoreType.DMA((6,)),
            pltpu.SemaphoreType.DMA((2, 2)),
            pltpu.SemaphoreType.DMA((2, 2)),
            pltpu.SemaphoreType.DMA((3, N)),
            pltpu.SemaphoreType.DMA((2, 2, 4, 2)),
            pltpu.SemaphoreType.DMA((2, 2, 4, 2)),
        ],
        compiler_params=pltpu.CompilerParams(collective_id=0, has_side_effects=True, vmem_limit_bytes=62000000),
    )(pair_wave, jnp.transpose(legendre, (1, 0, 2)), jnp.transpose(coefs, (1, 0, 2)))


def solution(mesh):
    split = Mesh(mesh.devices.reshape(N, N, 4, 2), ("y", "z", "x", "c"))
    placed = (P(), P(("x", "c"), ("y", "z"), None), P(("x", "c"), ("y", "z"), None))
    return jax.shard_map(
        body, mesh=split, in_specs=placed, out_specs=P(("y", "z", "x", "c"), None), check_vma=False
    )
```

```python
import math

import jax
import jax.numpy as jnp
import numpy as np
from jax import lax
from jax.experimental import pallas as pl
from jax.experimental.pallas import tpu as pltpu
from jax.sharding import Mesh
from jax.sharding import PartitionSpec as P

DEG = 720
LON = 1440
HALF = LON // 2
CH = 84
LAT = 10
SLOTS = 45
PER = 6
N = 8
ROWS = 105
PADDED = 112
RR = 768
F32 = jnp.float32
BF = jnp.bfloat16
MESH_ID = pl.DeviceIdType.MESH
FAR_FIRST = (4, 3, 5, 2, 6, 1, 7)
STRIDE = 88
BEFORE = (1, 7, 4)
BETWEEN = ((2, 6), (3, 5))
EARLY = 8
LATER = 8
SHRINK = 0.9999


def half_angle_fit():
    t = np.cos(np.linspace(0, np.pi, 4001)) * (np.pi / 2)
    sin_c = np.linalg.lstsq(np.stack([t ** (2 * i + 1) for i in range(5)], 1), np.sin(t), rcond=None)[0]
    cos_c = np.linalg.lstsq(np.stack([t ** (2 * i) for i in range(6)], 1), np.cos(t), rcond=None)[0]
    return [float(v) for v in sin_c], [float(v) for v in cos_c]


SIN_C, COS_C = half_angle_fit()


def horner(coefs, square):
    total = jnp.full_like(square, coefs[-1])
    for value in coefs[-2::-1]:
        total = total * square + value
    return total


def wave_rows(waves, weight, lon_at):
    product = waves * lon_at
    turns = jnp.round(product * (1.0 / LON))
    half = (product - turns * float(LON)) * (math.pi / LON)
    square = half * half
    sine = half * horner(SIN_C, square)
    cosine = horner(COS_C, square)
    twice = (2.0 * weight) * sine
    return weight - twice * sine, -twice * cosine


def split_bf16(x):
    high = x.astype(BF)
    return high, (x - high.astype(F32)).astype(BF)


def natural_rows():
    lane = lax.broadcasted_iota(jnp.int32, (1, RR), 1).astype(F32)
    z_at = jnp.floor((lane + 0.5) * (1.0 / 96))
    rest = lane - 96.0 * z_at
    y_at = jnp.floor((rest + 0.5) * (1.0 / 12))
    return lane, (8.0 * y_at + z_at) * 12.0 + rest - 12.0 * y_at


def kernel(
    pw_hbm, leg_hbm, cf_hbm, out,
    pw, leg, cf, perm, cbuf, csend, crecv, gat, lbuf, lsend, lrecv, ltail, fbuf, fsend, frecv, fdec, ucol, bas,
    in_sem, own_sem, csem, lsem, fsem, ring_s, ring_r,
):
    y, z = lax.axis_index("y"), lax.axis_index("z")
    m = 2 * lax.axis_index("x") + lax.axis_index("c")
    along, across = (z, y), (y, z)

    def device(kind, along_at, across_at, m_at):
        place = (across_at, along_at) if kind == 0 else (along_at, across_at)
        return (*place, m_at // 2, m_at % 2)

    barrier = pltpu.get_barrier_semaphore()
    peers = [device(kind, (along[kind] + t) % N, across[kind], m) for t in FAR_FIRST for kind in range(2)]
    peers += [device(0, z, y, (m + t) % N) for t in FAR_FIRST]
    for peer in peers:
        pl.semaphore_signal(barrier, inc=1, device_id=peer, device_id_type=MESH_ID)
    cf_in = pltpu.make_async_copy(cf_hbm, cf, in_sem.at[0])
    leg_in = pltpu.make_async_copy(leg_hbm, leg, in_sem.at[1])
    pw_in = pltpu.make_async_copy(pw_hbm, pw, in_sem.at[2])
    cf_in.start()
    leg_in.start()
    pw_in.start()

    lane_row, natural = natural_rows()

    @pl.loop(0, 48)
    def _(block):
        row = lax.broadcasted_iota(jnp.int32, (16, RR), 0).astype(F32) + (16 * block).astype(F32)
        perm[pl.ds(pl.multiple_of(block * 16, 16), 16), :] = jnp.where(row == natural, 1.0, 0.0).astype(BF)

    def slot_tile(ref, row, j):
        count = min(8, SLOTS - 8 * j)
        tile = ref[row, 8 * j : 8 * j + count, :].astype(F32)
        if count < 8:
            tile = jnp.concatenate([tile, jnp.zeros((8 - count, tile.shape[1]), F32)], 0)
        return tile

    cf_in.wait()
    for r in range(12):
        for g in range(2):
            tiles = [slot_tile(cf, r, 3 * g + k) for k in range(3)]
            at = 8 * (48 * g + 4 * r)
            for k in range(3):
                cbuf[at + 8 * k : at + 8 * k + 8, :] = tiles[k][:, :128]
            rest = [t[:, 128:] for t in tiles] + [jnp.zeros((8, 8), F32)]
            cbuf[at + 24 : at + 32, :] = jnp.concatenate(rest, 1)
    for g in range(2):
        for d in range(N):
            csend[g, d] = cbuf[pl.ds(384 * g + d, 48, stride=8), :].astype(BF)

    def put_leg(kind, i, k, tile):
        at = 240 * kind + 8 * (8 * k + i if i < 8 else 24 + 2 * k + i - 8)
        for l in range(6):
            lbuf[l, at : at + 8, :] = tile[:, 128 * l : 128 * l + 128]

    def pack_leg(kind):
        for d in range(N):
            for l in range(6):
                rows = lbuf[l, pl.ds(240 * kind + d, 30, stride=8), :]
                lsend[kind, d, :, 128 * l : 128 * l + 128] = rows.astype(BF)

    leg_in.wait()
    for i in range(LAT):
        for k in range(3):
            put_leg(0, i, k, slot_tile(leg, i, k))
    pack_leg(0)

    pl.semaphore_wait(barrier, len(peers))

    own_c = pltpu.make_async_copy(
        csend.at[0, along[0]], crecv.at[0, along[0]], own_sem.at[0]
    ), pltpu.make_async_copy(csend.at[1, along[1]], crecv.at[1, along[1]], own_sem.at[1])
    for t in FAR_FIRST:
        for kind in range(2):
            to = (along[kind] + t) % N
            pltpu.make_async_remote_copy(
                csend.at[kind, to], crecv.at[kind, along[kind]], csem.at[0, kind], csem.at[1, kind],
                device_id=device(kind, to, across[kind], m), device_id_type=MESH_ID,
            ).start()
    own_c[0].start()
    own_c[1].start()

    def send_leg(t):
        for kind in range(2):
            to = (along[kind] + t) % N
            pltpu.make_async_remote_copy(
                lsend.at[kind, to], lrecv.at[kind, t], lsem.at[0, kind], lsem.at[1, kind],
                device_id=device(kind, to, across[kind], m), device_id_type=MESH_ID,
            ).start()

    rows = [jnp.concatenate([slot_tile(leg, i, 3 + k) for k in range(3)], 0).astype(BF) for i in range(LAT)]
    moved = jnp.dot(jnp.concatenate(rows, 0), perm[...], preferred_element_type=F32)
    for i in range(LAT):
        for k in range(3):
            put_leg(1, i, k, moved[24 * i + 8 * k : 24 * i + 8 * k + 8])
    pack_leg(1)
    for t in BEFORE:
        send_leg(t)
    pw_in.wait()

    @pl.loop(0, PER * N)
    def _(tile):
        first = SLOTS * (tile % N) + 8 * (tile // N)
        rows = [jnp.full((1, 128), pw[jnp.minimum(first + d, 359)].astype(F32)) for d in range(8)]
        ucol[pl.ds(pl.multiple_of(tile * 8, 8), 8), :] = jnp.concatenate(rows, 0)

    lane = lax.broadcasted_iota(jnp.int32, (16, 128), 1).astype(F32)

    def make_basis(first, last):
        @pl.loop(first, last)
        def _(block):
            at = pl.multiple_of(block * 16, 16)
            u = ucol[pl.ds(at, 16), :]
            odd = u - 2.0 * jnp.floor(u * 0.5) > 0.5
            even_wave = jnp.where(odd, float(DEG - 1) - u, u)
            weight = jnp.where(even_wave == 0.0, 1.0, 2.0)
            for h, (wave, wt) in enumerate(((even_wave, weight), (float(DEG - 1) - even_wave, 2.0))):
                for l in range(6):
                    pair = wave_rows(wave, wt, lane + 128.0 * l)
                    for e in range(2):
                        high, low = split_bf16(pair[e])
                        to = pl.multiple_of(384 * e + at, 16)
                        bas[h, 0, pl.ds(to, 16), 128 * l : 128 * l + 128] = high
                        bas[h, 1, pl.ds(to, 16), 128 * l : 128 * l + 128] = low

    own_l = [
        pltpu.make_async_copy(lsend.at[kind, along[kind]], lrecv.at[kind, 0], own_sem.at[2 + kind])
        for kind in range(2)
    ]
    own_l[0].start()
    own_l[1].start()
    make_basis(0, EARLY)

    def wait_bytes(ref, sem):
        pltpu.make_async_copy(ref, ref, sem).wait()

    def ring(kind, way, step, half):
        own, back, on = across[kind], min(step, 2), 1 + step // 3
        origin = (own - back + N) % N if way == 0 else (own + back) % N
        part = gat.at[kind, origin, pl.ds(2 * half, 2)]
        to = (own + on) % N if way == 0 else (own + N - on) % N
        return pltpu.make_async_remote_copy(
            part, part, ring_s.at[kind, way, step, half], ring_r.at[kind, way, step, half],
            device_id=device(kind, along[kind], to, m), device_id_type=MESH_ID,
        )

    for kind in range(2):
        own_c[kind].wait()
        wait_bytes(crecv.at[kind, pl.ds(0, 7)], csem.at[1, kind])
        for s in range(N):
            cbuf[48 * s : 48 * s + 48, :] = crecv[kind, s].astype(F32)
        for blk in range(4):
            gat[kind, across[kind], blk] = cbuf[pl.ds(blk, 96, stride=4), :].astype(BF)
        for half in range(2):
            for way in range(2):
                ring(kind, way, 0, half).start()
    for step in range(1, 3):
        for t in BETWEEN[step - 1]:
            send_leg(t)
        make_basis(EARLY + LATER * (step - 1), min(24, EARLY + LATER * step))
        for half in range(2):
            for kind in range(2):
                for way in range(2):
                    ring(kind, way, step - 1, half).wait_recv()
                    if step == 2 and way == half:
                        ring(kind, way, 3, half).start()
                    ring(kind, way, step, half).start()
    for kind in range(2):
        own_l[kind].wait()
        wait_bytes(lrecv.at[kind, pl.ds(0, 7)], lsem.at[1, kind])
        for t in range(N):
            for l in range(6):
                ltail[kind, l, 8 * t : 8 * t + 6, :] = lrecv[kind, t, 24:30, 128 * l : 128 * l + 128].astype(F32)
    for kind in range(2):
        for way in range(2):
            for half in range(2):
                ring(kind, way, 2, half).wait_recv()
            ring(kind, way, 3, way).wait_recv()

    lane80 = lax.broadcasted_iota(jnp.int32, (80, 128), 1)
    for j in range(PER):
        kind, k = divmod(j, 3)
        u = pw[SLOTS * m + jnp.minimum(8 * j + along[kind], SLOTS - 1)]
        row_at = natural if kind else lane_row
        low = (row_at < (DEG - u).astype(F32)).astype(F32)
        high = (row_at <= float(DEG)).astype(F32) - low
        swap = lax.rem(u, 2).astype(F32)
        masks = [(low + swap * (high - low)).astype(BF), (high + swap * (low - high)).astype(BF)]
        main = lrecv[kind, :, 8 * k : 8 * k + 8, :].reshape(64, RR)
        tail = [[ltail[kind, l, pl.ds(2 * k + n, 8, stride=8), :] for l in range(6)] for n in range(2)]
        tail = jnp.concatenate([jnp.concatenate(t, 1) for t in tail], 0)
        table = jnp.concatenate([main, tail.astype(BF)], 0)
        lhs = jnp.concatenate([table * masks[0], table * masks[1]], 0)
        rhs = jnp.concatenate([gat[kind, :, k].reshape(RR, 128), gat[kind, :, 3].reshape(RR, 128)], 1)
        sums = jnp.dot(lhs, rhs, preferred_element_type=F32)
        for h in range(2):
            first = sums[80 * h : 80 * h + 80, :128]
            second = sums[80 * h : 80 * h + 80, 128:]
            imag = jnp.where(
                lane80 < 44, pltpu.roll(first, 44, axis=1), pltpu.roll(second, (44 - 40 * k) % 128, axis=1)
            )
            for e, value in enumerate((first, imag)):
                at = (16 * kind + 8 * h + 3 * e + k) * STRIDE
                fbuf[at : at + 80, :] = jnp.where(lane80 < CH, value, 0.0)

    lane8 = lax.broadcasted_iota(jnp.int32, (8, 128), 1)

    def lats_of(t):
        at = [8 * t + i if i < 8 else 64 + 8 * (i - 8) + t for i in range(LAT)]
        return [fbuf[pl.ds(first, 32, stride=STRIDE), :] for first in at]

    def level_of(t):
        most = [jnp.abs(value) for value in lats_of(t)]
        while len(most) > 1:
            most = [jnp.maximum(a, b) for a, b in zip(most[::2], most[1::2])] + most[len(most) // 2 * 2 :]
        return jnp.ceil(jnp.log2(jnp.maximum(jnp.max(most[0], axis=1, keepdims=True), 1e-30)))

    def words(value):
        whole = value.astype(jnp.int32)
        return [(whole[at : at + 8] & 0xFFFF) | (whole[at + 8 : at + 16] << 16) for at in (0, 16)]

    def pack(t):
        gain = jnp.exp2(15.0 - levels[t]) * SHRINK
        lats = [words(jnp.round(value * gain)) for value in lats_of(t)]
        level = words(jnp.broadcast_to(levels[t], (32, 128)))
        for k in range(N):
            i, skip = k + k // 4, 21 * (k % 4)
            inside = (lane8 >= skip) & (lane8 < CH)
            for kind in range(2):
                window = jnp.where(inside, lats[i][kind], pltpu.roll(lats[i + 1][kind], CH, axis=1))
                window = jnp.where(lane8 == (skip + 127) % 128, level[kind], window)
                fsend[t, k, kind] = window[:PER]

    def send_f(t):
        for n in range(0 if t else 1, N):
            m_to = (m + n) % N
            for kind in range(2):
                to = (along[kind] - t + N) % N
                pltpu.make_async_remote_copy(
                    fsend.at[t, m_to, kind], frecv.at[kind, m * N + along[kind]], fsem.at[0, kind], fsem.at[1 + kind, t],
                    device_id=device(kind, to, across[kind], m_to), device_id_type=MESH_ID,
                ).start()

    order = FAR_FIRST + (0,)
    levels = {t: level_of(t) for t in order}
    for n, t in enumerate(order):
        pack(t)
        if n >= 1:
            send_f(order[n - 1])
    send_f(0)
    own_f = [
        pltpu.make_async_copy(fsend.at[0, m, kind], frecv.at[kind, m * N + along[kind]], own_sem.at[4 + kind])
        for kind in range(2)
    ]
    own_f[0].start()
    own_f[1].start()

    for kind in range(2):
        wait_bytes(csend.at[kind, pl.ds(0, 7)], csem.at[0, kind])
        wait_bytes(lsend.at[kind, pl.ds(0, 7)], lsem.at[0, kind])
        for way in range(2):
            for step in range(4):
                for half in range(2):
                    if step < 3 or way == half:
                        ring(kind, way, step, half).wait_send()

    turn = lax.rem(128 - 21 * lax.rem(m, 4), 128)
    totals = [[0.0, 0.0] for l in range(3)]
    for kind in range(2):
        own_f[kind].wait()
        for t in order:
            wait_bytes(frecv.at[kind, pl.ds(0, 8 if t else 7)], fsem.at[1 + kind, t])
            source = (along[kind] + t) % N
            for n in range(N):
                coded = pltpu.roll(frecv[kind, 8 * n + source], turn, axis=1)
                at = pl.multiple_of((64 * kind + 8 * n + source) * 8, 8)
                fdec[pl.ds(at, PER), :] = ((coded << 16) >> 16).astype(F32)
                fdec[pl.ds(1024 + at, PER), :] = (coded >> 16).astype(F32)
        for h in range(2):
            at = [1024 * h + 512 * kind + n for n in range(PER)]
            rows = jnp.concatenate([fdec[pl.ds(first, 64, stride=8), :] for first in at], 0)
            rows = jnp.transpose(rows)
            rows = rows[:PADDED] * (jnp.exp2(rows[127:128, :] - 15.0) * (1.0 / SHRINK))
            high, low = split_bf16(rows)
            both = jnp.concatenate([high, low], 0)
            for l in range(3):
                at = slice(256 * l, 256 * l + 256)
                base = [
                    jnp.concatenate([bas[h, n, 384 * e + 192 * kind : 384 * e + 192 * kind + 192, at] for e in range(2)], 0)
                    for n in range(2)
                ]
                wide = jnp.dot(both, base[0], preferred_element_type=F32)
                part = wide[:PADDED] + wide[PADDED:] + jnp.dot(high, base[1], preferred_element_type=F32)
                totals[l][h] = totals[l][h] + part
    for l in range(3):
        part = totals[l]
        count = min(256, HALF - 256 * l)
        out[:, 256 * l : 256 * l + count] = (part[0] + part[1])[:ROWS, :count]
        out[:, HALF + 256 * l : HALF + 256 * l + count] = (part[0] - part[1])[:ROWS, :count]
    for kind in range(2):
        wait_bytes(frecv.at[kind, pl.ds(0, 63)], fsem.at[0, kind])


def body(pair_wave, legendre, coefs):
    return pl.pallas_call(
        kernel,
        out_shape=pltpu.VMEM((ROWS, LON), F32),
        in_specs=[
            pl.BlockSpec(memory_space=pltpu.HBM),
            pl.BlockSpec(memory_space=pltpu.HBM),
            pl.BlockSpec(memory_space=pltpu.HBM),
        ],
        out_specs=pl.BlockSpec(memory_space=pltpu.VMEM),
        scratch_shapes=[
            pltpu.SMEM((360,), jnp.int32),
            pltpu.VMEM((LAT, SLOTS, RR), BF),
            pltpu.VMEM((12, SLOTS, 2 * CH), BF),
            pltpu.VMEM((RR, RR), BF),
            pltpu.VMEM((768, 128), F32),
            pltpu.VMEM((2, N, 48, 128), BF),
            pltpu.VMEM((2, N, 48, 128), BF),
            pltpu.VMEM((2, N, 4, 96, 128), BF),
            pltpu.VMEM((6, 480, 128), F32),
            pltpu.VMEM((2, N, 30, RR), BF),
            pltpu.VMEM((2, N, 30, RR), BF),
            pltpu.VMEM((2, 6, 64, 128), F32),
            pltpu.VMEM((32 * STRIDE, 128), F32),
            pltpu.VMEM((N, N, 2, PER, 128), jnp.int32),
            pltpu.VMEM((2, N * N, PER, 128), jnp.int32),
            pltpu.VMEM((2 * 2 * N * N * 8, 128), F32),
            pltpu.VMEM((384, 128), F32),
            pltpu.VMEM((2, 2, RR, RR), BF),
            pltpu.SemaphoreType.DMA((3,)),
            pltpu.SemaphoreType.DMA((6,)),
            pltpu.SemaphoreType.DMA((2, 2)),
            pltpu.SemaphoreType.DMA((2, 2)),
            pltpu.SemaphoreType.DMA((3, N)),
            pltpu.SemaphoreType.DMA((2, 2, 4, 2)),
            pltpu.SemaphoreType.DMA((2, 2, 4, 2)),
        ],
        compiler_params=pltpu.CompilerParams(collective_id=0, has_side_effects=True, vmem_limit_bytes=62000000),
    )(pair_wave, jnp.transpose(legendre, (1, 0, 2)), jnp.transpose(coefs, (1, 0, 2)))


def solution(mesh):
    split = Mesh(mesh.devices.reshape(N, N, 4, 2), ("y", "z", "x", "c"))
    placed = (P(), P(("x", "c"), ("y", "z"), None), P(("x", "c"), ("y", "z"), None))
    return jax.shard_map(
        body, mesh=split, in_specs=placed, out_specs=P(("y", "z", "x", "c"), None), check_vma=False
    )
```
